32 devices in a mesh: wide: 4 (over z), tp: 2 (over y), rep: 4 (over x, core).
Axes of the slice: x: 2, y: 2, z: 4, core: 2. Of those that a mesh axis runs over, the one named last changes fastest.
Arguments:
- activations: bfloat16 [32768, 8192], P('rep', 'wide'), may hold values from -6 to 6
- value_grads: bfloat16 [32768, 1024], P('rep', 'tp'), may hold values from -24 to 24
- seq_lengths: int32 [32], P('rep'), may hold values from 128 to 1024
- master: float32 [8192, 1024], P(('wide', 'rep'), 'tp'), may hold values from -0.0625 to 0.0625
- first_moment: float32 [8192, 1024], P(('wide', 'rep'), 'tp'), may hold values from -3 to 3
- second_moment: float32 [8192, 1024], P(('wide', 'rep'), 'tp'), may hold values from 0.05 to 2
- hidden: bfloat16 [4, 64, 8192], P(None, ('wide', 'rep')), may hold values from -6 to 6
- queries: bfloat16 [4, 64, 8192], P(None, ('wide', 'rep'), 'tp'), may hold values from -200 to 200
- new_keys: bfloat16 [4, 64, 1024], P(None, ('wide', 'rep'), 'tp'), may hold values from -6 to 6
- cache_keys: bfloat16 [64, 256, 1024], P(('wide', 'rep'), None, 'tp'), may hold values from -6 to 6
- cache_values: bfloat16 [64, 256, 1024], P(('wide', 'rep'), None, 'tp'), may hold values from -6 to 6
- cache_lengths: int32 [64], P(('wide', 'rep')), may hold values from 2 to 256
Outputs:
- new_master: float32 [8192, 1024], P(('wide', 'rep'), 'tp')
- new_first: float32 [8192, 1024], P(('wide', 'rep'), 'tp')
- new_second: float32 [8192, 1024], P(('wide', 'rep'), 'tp')
- new_values: bfloat16 [4, 64, 1024], P(None, ('wide', 'rep'), 'tp')
- attended: bfloat16 [4, 64, 8192], P(None, ('wide', 'rep'), 'tp')
The draws below stay inside these ranges and needn't reach their ends.
All inputs are finite; a program needn't handle non-finite values.
Results may differ from the reference program's by a relative error of at most 0.012.
Values may be sent and summed in bfloat16 or wider, within the bound.
No kernel may reach another device: no remote copies, remote signals or barrier semaphores. Data moves between devices by JAX's collectives and lax.ppermute only.
A program may use at most 128 MiB of HBM per device.

```python
import math
import jax
import jax.numpy as jnp
from jax import lax

D = 8192
HEADS = 64
KV_HEADS = 8
HEAD = 128
QUANT = 128
STEPS = 4
SEQLEN = 1024
CACHE = 256
KVD = 1024
TOKENS = 32768
SEQS = 32
ROWS = 64


def entries(key):
    drawn_keys = jnp.clip(jax.random.normal(jax.random.fold_in(key, 101), (ROWS, CACHE, KVD), jnp.float32), -6.0, 6.0)
    return drawn_keys


def draw_cache_keys(key, part):
    drawn_keys = entries(key)
    return drawn_keys.astype(jnp.bfloat16)


def draw_queries(key, part):
    drawn = jnp.clip(jax.random.normal(jax.random.fold_in(key, 104), (STEPS, ROWS, HEADS * HEAD), jnp.float32), -6.0, 6.0)
    return drawn.astype(jnp.bfloat16)


def set_ends(values, own_key, least, top_value):
    extent = values.shape
    spot = [jax.random.randint(jax.random.fold_in(own_key, axis), (), 0, extent[axis]) for axis in range(len(extent))]
    values = values.at[tuple(spot)].set(least)
    longest = extent.index(max(extent))
    spot[longest] = (spot[longest] + 1) % extent[longest]
    return values.at[tuple(spot)].set(top_value)


def steps_of(stream_key, dims, pieces, smallest, high):
    def one(dim, blocks):
        draws = jax.random.uniform(jax.random.fold_in(jax.random.fold_in(stream_key, 6), dim), (blocks,), jnp.float32, smallest / len(pieces), high / len(pieces))
        return jnp.repeat(jnp.exp(draws), dims[dim] // blocks).reshape((-1,) + (1,) * (len(dims) - dim - 1))

    factor_of = one(*pieces[0])
    for cut in pieces[1:]:
        factor_of = factor_of * one(*cut)
    return factor_of


def normal_values(rng, shape, width, limit, shards=(), kind=jnp.bfloat16):
    values = jax.random.normal(rng, shape, jnp.float32) * width
    if len(shards) > 0:
        values = steps_of(rng, shape, shards, -0.22, 0.18) * values
    return jnp.clip(values, min=-limit, max=limit).astype(kind)


def setup_inputs(seed: int = 0) -> dict:
    key_list = jax.random.split(jax.random.key(seed), 13)
    activations = normal_values(key_list[0], (TOKENS, D), 1.0, 6.0, ((0, 4), (1, 4)))
    value_grads = normal_values(key_list[1], (TOKENS, KVD), 4.0, 24.0, ((0, 4), (1, 2)))
    seq_lengths = set_ends(jax.random.randint(key_list[2], (SEQS,), SEQLEN // 8, SEQLEN + 1), jax.random.fold_in(key_list[2], 1), SEQLEN // 8, SEQLEN).astype(jnp.int32)
    master = normal_values(key_list[3], (D, KVD), D ** -0.5, 0.0625, ((0, 16), (1, 2)), jnp.float32)
    first_moment = normal_values(key_list[4], (D, KVD), 0.5, 3.0, ((0, 16), (1, 2)), jnp.float32)
    second_moment = jnp.clip(jnp.exp(math.log(2.0) - 3.6888794 * jax.random.uniform(key_list[5], (D, KVD), jnp.float32) ** steps_of(key_list[5], (D, KVD), ((0, 16), (1, 2)), -0.2, 0.2)), 0.05, 2.0)
    hidden = normal_values(key_list[6], (STEPS, ROWS, D), 1.0, 6.0, ((1, 16),))
    queries = draw_queries(jax.random.fold_in(key_list[12], 71), 0)
    new_keys = normal_values(key_list[8], (STEPS, ROWS, KVD), 1.0, 6.0, ((1, 16), (2, 2)))
    cache_keys = draw_cache_keys(jax.random.fold_in(key_list[12], 71), 0)
    cache_values = normal_values(key_list[10], (ROWS, CACHE, KVD), 1.0, 6.0, ((0, 16), (2, 2)))
    cache_lengths = set_ends(jax.random.randint(key_list[11], (ROWS,), 2, CACHE + 1), jax.random.fold_in(key_list[11], 1), 2, CACHE).astype(jnp.int32)
    return dict(activations=activations, value_grads=value_grads, seq_lengths=seq_lengths, master=master, first_moment=first_moment, second_moment=second_moment, hidden=hidden, queries=queries, new_keys=new_keys, cache_keys=cache_keys, cache_values=cache_values, cache_lengths=cache_lengths)


beta_one = 0.9
beta_two = 0.95
learn_rate = 0.001
weight_decay = 0.1
epsilon = 1e-08
steps_done = 10.0
quant_top = 448.0
scale_epsilon = 1e-06

def quantize(weights):
    row_count, col_count = weights.shape
    tiled = weights.reshape(row_count, col_count // QUANT, QUANT)
    largest = lax.optimization_barrier(jnp.max(jnp.abs(tiled), axis=2))
    scales = ((largest + scale_epsilon) / quant_top).astype(jnp.bfloat16)
    quantized = (tiled / scales.astype(jnp.float32)[:, :, None]).astype(jnp.bfloat16)
    return (quantized.reshape(row_count, col_count), scales)

def dequantize(quantized, scales):
    row_count, col_count = quantized.shape
    tiled = quantized.astype(jnp.float32).reshape(row_count, col_count // QUANT, QUANT)
    return (tiled * scales.astype(jnp.float32)[:, :, None]).reshape(row_count, col_count)

def reference(activations, value_grads, seq_lengths, master, first_moment, second_moment, hidden, queries, new_keys, cache_keys, cache_values, cache_lengths):
    position = jnp.arange(SEQLEN, dtype=jnp.int32)
    lengths = seq_lengths.astype(jnp.float32)
    token_weight = jnp.where(position[None, :] < seq_lengths[:, None], 1.0 / lengths[:, None], 0.0)
    weighted = (value_grads.astype(jnp.float32).reshape(SEQS, SEQLEN, KVD) * token_weight[:, :, None]).astype(jnp.bfloat16)
    weighted = weighted.reshape(TOKENS, KVD)
    gradient = lax.dot_general(activations, weighted, (((0,), (0,)), ((), ())), preferred_element_type=jnp.float32)
    new_first = beta_one * first_moment + (1.0 - beta_one) * gradient
    new_second = beta_two * second_moment + (1.0 - beta_two) * gradient * gradient
    corrected_first = new_first / (1.0 - beta_one ** steps_done)
    corrected_second = new_second / (1.0 - beta_two ** steps_done)
    new_master = master - learn_rate * (corrected_first / (jnp.sqrt(corrected_second) + epsilon) + weight_decay * master)
    quantized, scales = quantize(new_master)
    weight_used = dequantize(quantized, scales)
    flat_hidden = hidden.reshape(STEPS * ROWS, D).astype(jnp.float32)
    projected = jnp.dot(flat_hidden, weight_used, precision=lax.Precision.HIGHEST, preferred_element_type=jnp.float32)
    new_values = projected.astype(jnp.bfloat16).reshape(STEPS, ROWS, KVD)
    group = HEADS // KV_HEADS
    score_scale = HEAD ** (-0.5)
    keys_cache = cache_keys.astype(jnp.float32).reshape(ROWS, CACHE, KV_HEADS, HEAD)
    values_cache = cache_values.astype(jnp.float32).reshape(ROWS, CACHE, KV_HEADS, HEAD)
    keys_new = new_keys.astype(jnp.float32).reshape(STEPS, ROWS, KV_HEADS, HEAD)
    values_new = new_values.astype(jnp.float32).reshape(STEPS, ROWS, KV_HEADS, HEAD)
    slots = jnp.arange(CACHE, dtype=jnp.int32)
    cache_live = slots[None, :] < cache_lengths[:, None]
    outputs = []
    for moment in range(STEPS):
        query = queries[moment].astype(jnp.float32).reshape(ROWS, KV_HEADS, group, HEAD)
        scores_cache = jnp.einsum('bgrd,bjgd->bgrj', query, keys_cache) * score_scale
        scores_cache = jnp.where(cache_live[:, None, None, :], scores_cache, -jnp.inf)
        scores_new = jnp.einsum('bgrd,tbgd->bgrt', query, keys_new[:moment + 1]) * score_scale
        highest = jnp.maximum(lax.optimization_barrier(jnp.max(scores_cache, axis=3)), lax.optimization_barrier(jnp.max(scores_new, axis=3)))
        exp_cache = jnp.exp(scores_cache - highest[..., None])
        exp_new = jnp.exp(scores_new - highest[..., None])
        totals = lax.optimization_barrier(jnp.sum(exp_cache, axis=3)) + lax.optimization_barrier(jnp.sum(exp_new, axis=3))
        probs_cache = lax.optimization_barrier((exp_cache / totals[..., None]).astype(jnp.bfloat16)).astype(jnp.float32)
        probs_new = lax.optimization_barrier((exp_new / totals[..., None]).astype(jnp.bfloat16)).astype(jnp.float32)
        mixed = jnp.einsum('bgrj,bjgd->bgrd', probs_cache, values_cache)
        mixed = mixed + jnp.einsum('bgrt,tbgd->bgrd', probs_new, values_new[:moment + 1])
        outputs.append(mixed.astype(jnp.bfloat16).reshape(ROWS, HEADS * HEAD))
    attended = jnp.stack(outputs, axis=0)
    return (new_master, new_first, new_second, new_values, attended)
```

```python
import functools

import jax
import jax.numpy as jnp
from jax import lax
from jax.experimental import pallas as pl
from jax.experimental.pallas import tpu as pltpu
from jax.sharding import PartitionSpec as P

HEADS = 64
KV_HEADS = 8
HEAD = 128
QUANT = 128


beta_one = 0.9
beta_two = 0.95
learn_rate = 0.001
weight_decay = 0.1
epsilon = 1e-08
steps_done = 10.0
quant_top = 448.0
scale_epsilon = 1e-06


def quantize(weights):
    row_count, col_count = weights.shape
    tiled = weights.reshape(row_count, col_count // QUANT, QUANT)
    largest = jnp.max(jnp.abs(tiled), axis=2)
    scales = ((largest + scale_epsilon) / quant_top).astype(jnp.bfloat16)
    quantized = (tiled / scales.astype(jnp.float32)[:, :, None]).astype(jnp.bfloat16)
    return (quantized.reshape(row_count, col_count), scales)


def dequantize(quantized, scales):
    row_count, col_count = quantized.shape
    tiled = quantized.astype(jnp.float32).reshape(row_count, col_count // QUANT, QUANT)
    return (tiled * scales.astype(jnp.float32)[:, :, None]).reshape(row_count, col_count)


def on_device_plain(
    activations,
    value_grads,
    seq_lengths,
    master,
    first_moment,
    second_moment,
    hidden,
    queries,
    new_keys,
    cache_keys,
    cache_values,
    cache_lengths,
):
    seq_count = seq_lengths.shape[0]
    token_count, col_count = value_grads.shape
    seq_span = token_count // seq_count
    position = jnp.arange(seq_span, dtype=jnp.int32)
    lengths = seq_lengths.astype(jnp.float32)
    token_weight = jnp.where(position[None, :] < seq_lengths[:, None], 1.0 / lengths[:, None], 0.0)
    weighted = (
        value_grads.astype(jnp.float32).reshape(seq_count, seq_span, col_count)
        * token_weight[:, :, None]
    ).astype(jnp.bfloat16)
    weighted = weighted.reshape(token_count, col_count)
    gradient = lax.psum_scatter(
        lax.dot_general(
            activations, weighted, (((0,), (0,)), ((), ())), preferred_element_type=jnp.float32
        ),
        "rep",
        scatter_dimension=0,
        tiled=True,
    )
    new_first = beta_one * first_moment + (1.0 - beta_one) * gradient
    new_second = beta_two * second_moment + (1.0 - beta_two) * gradient * gradient
    corrected_first = new_first / (1.0 - beta_one**steps_done)
    corrected_second = new_second / (1.0 - beta_two**steps_done)
    new_master = master - learn_rate * (
        corrected_first / (jnp.sqrt(corrected_second) + epsilon) + weight_decay * master
    )
    quantized, scales = quantize(new_master)
    step_count, row_local, width = hidden.shape
    score_scale = HEAD ** (-0.5)
    group = HEADS // KV_HEADS
    kv_local = col_count // HEAD
    query = queries.reshape(step_count, row_local, kv_local, group, HEAD)
    keys_cache = cache_keys.reshape(row_local, cache_keys.shape[1], kv_local, HEAD)
    values_cache = cache_values.reshape(row_local, cache_values.shape[1], kv_local, HEAD)
    keys_new = new_keys.reshape(step_count, row_local, kv_local, HEAD)
    slots = jnp.arange(cache_keys.shape[1], dtype=jnp.int32)
    cache_live = slots[None, :] < cache_lengths[:, None]
    scores_cache = (
        jnp.einsum("sbgrd,bjgd->sbgrj", query, keys_cache, preferred_element_type=jnp.float32)
        * score_scale
    )
    scores_cache = jnp.where(cache_live[None, :, None, None, :], scores_cache, -jnp.inf)
    scores_new = (
        jnp.einsum("sbgrd,tbgd->sbgrt", query, keys_new, preferred_element_type=jnp.float32)
        * score_scale
    )
    moments = jnp.arange(step_count, dtype=jnp.int32)
    earlier = moments[None, :] <= moments[:, None]
    scores_new = jnp.where(earlier[:, None, None, None, :], scores_new, -jnp.inf)
    highest = jnp.maximum(jnp.max(scores_cache, axis=4), jnp.max(scores_new, axis=4))
    exp_cache = jnp.exp(scores_cache - highest[..., None])
    exp_new = jnp.exp(scores_new - highest[..., None])
    totals = jnp.sum(exp_cache, axis=4) + jnp.sum(exp_new, axis=4)
    probs_cache = (exp_cache / totals[..., None]).astype(jnp.bfloat16)
    probs_new = (exp_new / totals[..., None]).astype(jnp.bfloat16)
    mixed_cache = jnp.einsum(
        "sbgrj,bjgd->sbgrd", probs_cache, values_cache, preferred_element_type=jnp.float32
    )
    wide_count = lax.axis_size("wide")
    rep_count = lax.axis_size("rep")
    block_rows = width // (wide_count * rep_count)
    arranged = hidden.reshape(step_count, row_local, wide_count, rep_count, block_rows)
    swapped = lax.all_to_all(arranged, "rep", split_axis=3, concat_axis=1, tiled=True)
    group_rows = rep_count * row_local
    flat_group = swapped.reshape(step_count * group_rows, wide_count * block_rows).astype(
        jnp.float32
    )
    quant_rows = lax.all_gather(quantized, "wide", axis=0, tiled=True)
    scale_rows = lax.all_gather(scales, "wide", axis=0, tiled=True)
    weight_rows = dequantize(quant_rows, scale_rows)
    partial_value = jnp.dot(
        flat_group, weight_rows, precision=lax.Precision.HIGHEST, preferred_element_type=jnp.float32
    )
    partial_value = partial_value.reshape(step_count, group_rows, col_count)
    projected = lax.psum_scatter(partial_value, "rep", scatter_dimension=1, tiled=True)
    new_values = projected.astype(jnp.bfloat16)
    values_new = new_values.reshape(step_count, row_local, kv_local, HEAD)
    mixed = mixed_cache + jnp.einsum(
        "sbgrt,tbgd->sbgrd", probs_new, values_new, preferred_element_type=jnp.float32
    )
    attended = mixed.astype(jnp.bfloat16).reshape(step_count, row_local, kv_local * group * HEAD)
    return (new_master, new_first, new_second, new_values, attended)


TOKEN_BLOCK = 256
BLOCKS_PER_STEP = 4
BUFFERS = 3


def live_blocks(lengths, block_of, limit_of, length_of, span):
    count = jnp.int32(0)
    per_seq = span // TOKEN_BLOCK
    for seq in range(lengths.shape[0]):
        length = lengths[seq]
        for part in range(per_seq):
            block_of[count] = seq * per_seq + part
            limit_of[count] = length - part * TOKEN_BLOCK
            length_of[count] = length
            count = count + jnp.where(length > part * TOKEN_BLOCK, 1, 0)
    for pad in range(BLOCKS_PER_STEP):
        block_of[count + pad] = 0
        limit_of[count + pad] = 0
        length_of[count + pad] = 1
    return lax.div(count + BLOCKS_PER_STEP - 1, BLOCKS_PER_STEP)


def start_acts(acts, buf, sem, block_of, step, slot, column, width):
    for part in range(BLOCKS_PER_STEP):
        first = pl.multiple_of(block_of[step * BLOCKS_PER_STEP + part] * TOKEN_BLOCK, TOKEN_BLOCK)
        pltpu.make_async_copy(
            acts.at[pl.ds(first, TOKEN_BLOCK), pl.ds(column, width)],
            buf.at[slot, pl.ds(part * TOKEN_BLOCK, TOKEN_BLOCK), :],
            sem.at[slot],
        ).start()


def wait_slot(source, buf, sem, slot):
    rows, cols = buf.shape[1:]
    pltpu.make_async_copy(source.at[pl.ds(0, rows), pl.ds(0, cols)], buf.at[slot], sem.at[slot]).wait()


def first_kernel(
    span,
    width,
    wide_count,
    rep_count,
    lengths,
    acts,
    grads,
    hidden,
    out,
    weighted,
    near,
    far,
    block_of,
    limit_of,
    length_of,
    acts_buf,
    grads_buf,
    turned,
    acc,
    flat,
    acts_sem,
    grads_sem,
    out_sem,
):
    rep = lax.axis_index("rep")
    here = lax.axis_index("wide")
    core = lax.rem(rep, 2)
    chip = lax.div(rep, 2)
    column = pl.multiple_of(((1 - chip) * 2 + (1 - core)) * width, width)
    steps = live_blocks(lengths, block_of, limit_of, length_of, span)
    step_rows = BLOCKS_PER_STEP * TOKEN_BLOCK
    cols = grads.shape[1]

    def start(step, slot):
        start_acts(acts, acts_buf, acts_sem, block_of, step, slot, column, width)
        start_acts(grads, grads_buf, grads_sem, block_of, step, slot, 0, cols)

    def store(step, slot):
        first = pl.multiple_of(step * step_rows, step_rows)
        return pltpu.make_async_copy(
            turned.at[slot], weighted.at[:, pl.ds(first, step_rows)], out_sem.at[slot]
        )

    for ahead in range(BUFFERS - 1):
        @pl.when(ahead < steps)
        def _():
            start(ahead, ahead)

    acc[...] = jnp.zeros_like(acc)
    count, rows, _ = hidden.shape
    for step in range(count):
        flat[step * rows : (step + 1) * rows, :] = hidden[step].astype(jnp.float32)
    for dx in range(2):
        target = far if dx else near
        for dz in range(wide_count):
            for dc in range(2):
                place = (here ^ dz) * rep_count + (chip ^ dx) * 2 + (core ^ dc)
                begin = pl.multiple_of(place * width, width)
                target[dz, dc] = flat[:, pl.ds(begin, width)].astype(jnp.bfloat16)

    def body(step, carry):
        slot = lax.rem(step, BUFFERS)
        later = step + BUFFERS - 1

        @pl.when(later < steps)
        def _():
            start(later, lax.rem(later, BUFFERS))

        wait_slot(grads, grads_buf, grads_sem, slot)

        @pl.when(step >= BUFFERS)
        def _():
            store(step - BUFFERS, slot).wait()

        for part in range(BLOCKS_PER_STEP):
            entry = step * BLOCKS_PER_STEP + part
            lanes = slice(part * TOKEN_BLOCK, (part + 1) * TOKEN_BLOCK)
            value = grads_buf[slot, lanes, :].astype(jnp.float32)
            length = jnp.full((1, cols), length_of[entry], jnp.int32).astype(jnp.float32)
            position = lax.broadcasted_iota(jnp.int32, value.shape, 0)
            scaled = jnp.where(position < limit_of[entry], value * (1.0 / length), 0.0)
            turned[slot, :, lanes] = scaled.astype(jnp.bfloat16).T
        store(step, slot).start()
        wait_slot(acts, acts_buf, acts_sem, slot)
        acc[...] += jnp.dot(turned[slot], acts_buf[slot], preferred_element_type=jnp.float32)
        return carry

    lax.fori_loop(0, steps, body, 0)
    for back in range(BUFFERS):
        @pl.when(steps > back)
        def _():
            last = steps - 1 - back
            store(last, lax.rem(last, BUFFERS)).wait()

    out[...] = acc[...].astype(jnp.bfloat16)


def later_kernel(
    span,
    width,
    own_chip,
    lengths,
    acts,
    weighted,
    *refs,
):
    if own_chip:
        ours, theirs, block_of, limit_of, length_of, acts_buf, turned, acc, acts_sem, turned_sem = refs
    else:
        arrived, ours, block_of, limit_of, length_of, acts_buf, turned, acc, acts_sem, turned_sem = refs
    rep = lax.axis_index("rep")
    core = lax.rem(rep, 2)
    chip = lax.div(rep, 2)
    if own_chip:
        column = pl.multiple_of(chip * 2 * width, 2 * width)
    else:
        column = pl.multiple_of(((1 - chip) * 2 + core) * width, width)
    taken = acts_buf.shape[2]
    steps = live_blocks(lengths, block_of, limit_of, length_of, span)
    step_rows = BLOCKS_PER_STEP * TOKEN_BLOCK

    def start(step, slot):
        start_acts(acts, acts_buf, acts_sem, block_of, step, slot, column, taken)
        first = pl.multiple_of(step * step_rows, step_rows)
        pltpu.make_async_copy(
            weighted.at[:, pl.ds(first, step_rows)], turned.at[slot], turned_sem.at[slot]
        ).start()

    for ahead in range(BUFFERS - 1):
        @pl.when(ahead < steps)
        def _():
            start(ahead, ahead)

    acc[...] = jnp.zeros_like(acc)

    def body(step, carry):
        slot = lax.rem(step, BUFFERS)
        later = step + BUFFERS - 1

        @pl.when(later < steps)
        def _():
            start(later, lax.rem(later, BUFFERS))

        wait_slot(weighted, turned, turned_sem, slot)
        wait_slot(acts, acts_buf, acts_sem, slot)
        acc[...] += jnp.dot(turned[slot], acts_buf[slot], preferred_element_type=jnp.float32)
        return carry

    lax.fori_loop(0, steps, body, 0)
    if own_chip:
        ours[...] = acc[:, pl.ds(pl.multiple_of(core * width, width), width)]
        theirs[...] = acc[:, pl.ds(pl.multiple_of((1 - core) * width, width), width)].astype(jnp.bfloat16)
    else:
        ours[...] = (acc[...] + arrived[...].astype(jnp.float32)).astype(jnp.bfloat16)


def update_kernel(
    own, from_core, from_chip, master, first, second, kept, sent,
    new_master, new_first, new_second, partial_kept, partial_sent,
):
    total = own[...] + from_core[...].astype(jnp.float32) + from_chip[...].astype(jnp.float32)
    gradient = total.T
    moved_first = beta_one * first[...] + (1.0 - beta_one) * gradient
    moved_second = beta_two * second[...] + (1.0 - beta_two) * gradient * gradient
    corrected_first = moved_first / (1.0 - beta_one**steps_done)
    corrected_second = moved_second / (1.0 - beta_two**steps_done)
    old = master[...]
    moved = old - learn_rate * (
        corrected_first / (jnp.sqrt(corrected_second) + epsilon) + weight_decay * old
    )
    new_first[...] = moved_first
    new_second[...] = moved_second
    new_master[...] = moved
    largest = jnp.max(jnp.abs(moved), axis=1, keepdims=True)
    scales = ((largest + scale_epsilon) / quant_top).astype(jnp.bfloat16).astype(jnp.float32)
    quantized = (moved / scales).astype(jnp.bfloat16).astype(jnp.float32)
    used = quantized * scales
    high = used.astype(jnp.bfloat16)
    low = (used - high.astype(jnp.float32)).astype(jnp.bfloat16)

    def project(rows):
        return jnp.dot(rows, high, preferred_element_type=jnp.float32) + jnp.dot(
            rows, low, preferred_element_type=jnp.float32
        )

    partial_sent[...] = project(sent[...]).astype(jnp.bfloat16)
    partial_kept[...] = project(kept[...])


def attention_kernel(lengths, queries, new_keys, cache_keys, cache_values, order, mixed, late, flat, keys):
    del order
    steps, seqs, _ = queries.shape
    slots = cache_keys.shape[1]
    kv_local = new_keys.shape[2] // HEAD
    group = HEADS // KV_HEADS
    lines = steps * seqs
    for step in range(steps):
        flat[step * seqs : (step + 1) * seqs, :] = queries[step].astype(jnp.float32)
        keys[step * seqs : (step + 1) * seqs, :] = new_keys[step].astype(jnp.float32)
    rows = group * lines

    def index(shape, axis):
        return lax.broadcasted_iota(jnp.int32, shape, axis)

    wide_shape = (rows, slots)
    seq_of = lax.rem(index(wide_shape, 0), seqs)
    limit = jnp.zeros(wide_shape, jnp.int32)
    for seq in range(seqs):
        limit = jnp.where(seq_of == seq, lengths[seq], limit)
    live = index(wide_shape, 1) < limit
    late_shape = (rows, lines)
    late_row = index(late_shape, 0)
    late_col = index(late_shape, 1)
    allowed = (lax.rem(late_row, seqs) == lax.rem(late_col, seqs)) & (
        lax.div(late_col, seqs) <= lax.rem(lax.div(late_row, seqs), steps)
    )
    score_scale = HEAD ** (-0.5)
    across = (((1,), (1,)), ((), ()))
    for head in range(kv_local):
        lanes = slice(head * HEAD, (head + 1) * HEAD)
        query = jnp.concatenate(
            [
                flat[:, (head * group + part) * HEAD : (head * group + part + 1) * HEAD]
                for part in range(group)
            ],
            axis=0,
        ).astype(jnp.bfloat16)
        scores = jnp.zeros(wide_shape, jnp.float32)
        for seq in range(seqs):
            one = lax.dot_general(
                query, cache_keys[seq, :, lanes], across, preferred_element_type=jnp.float32
            )
            scores = jnp.where(seq_of == seq, one, scores)
        scores = jnp.where(live, scores * score_scale, -jnp.inf)
        scores_new = (
            lax.dot_general(
                query, keys[:, lanes].astype(jnp.bfloat16), across, preferred_element_type=jnp.float32
            )
            * score_scale
        )
        scores_new = jnp.where(allowed, scores_new, -jnp.inf)
        highest = jnp.maximum(
            jnp.max(scores, axis=1, keepdims=True), jnp.max(scores_new, axis=1, keepdims=True)
        )
        exp_cache = jnp.exp(scores - highest)
        exp_new = jnp.exp(scores_new - highest)
        totals = jnp.sum(exp_cache, axis=1, keepdims=True) + jnp.sum(exp_new, axis=1, keepdims=True)
        probs = exp_cache / totals
        late[head] = (exp_new / totals).astype(jnp.bfloat16)
        result = jnp.zeros((rows, HEAD), jnp.float32)
        for seq in range(seqs):
            mine = jnp.where(seq_of == seq, probs, 0.0).astype(jnp.bfloat16)
            result = result + jnp.dot(
                mine, cache_values[seq, :, lanes], preferred_element_type=jnp.float32
            )
        mixed[head] = result


def finish_kernel(steps, seqs, *refs):
    mixed, late, own = refs[:3]
    arrived = refs[3:-3]
    new_values, attended, flat = refs[-3:]
    total = own[...]
    for block in arrived:
        total = total + block[...].astype(jnp.float32)
    values = total.astype(jnp.bfloat16)
    wide_values = values.astype(jnp.float32)
    lines = steps * seqs
    kv_local, rows, _ = mixed.shape
    group = rows // lines
    for head in range(kv_local):
        lanes = slice(head * HEAD, (head + 1) * HEAD)
        result = mixed[head] + jnp.dot(late[head], values[:, lanes], preferred_element_type=jnp.float32)
        for part in range(group):
            flat[:, (head * group + part) * HEAD : (head * group + part + 1) * HEAD] = result[
                part * lines : (part + 1) * lines, :
            ]
    for step in range(steps):
        new_values[step] = wide_values[step * seqs : (step + 1) * seqs, :].astype(jnp.bfloat16)
        attended[step] = flat[step * seqs : (step + 1) * seqs, :].astype(jnp.bfloat16)


HBM = pl.BlockSpec(memory_space=pltpu.HBM)
VMEM = pl.BlockSpec(memory_space=pltpu.VMEM)
SMEM = pl.BlockSpec(memory_space=pltpu.SMEM)
PARAMS = pltpu.CompilerParams(vmem_limit_bytes=40 * 1024 * 1024)


def on_device(
    activations,
    value_grads,
    seq_lengths,
    master,
    first_moment,
    second_moment,
    hidden,
    queries,
    new_keys,
    cache_keys,
    cache_values,
    cache_lengths,
):
    shape = jax.ShapeDtypeStruct
    bf16, f32 = jnp.bfloat16, jnp.float32
    wide_count = lax.axis_size("wide")
    rep_count = lax.axis_size("rep")
    tokens, cols = value_grads.shape
    seqs = seq_lengths.shape[0]
    span = tokens // seqs
    step_count, row_local, _ = hidden.shape
    lines = step_count * row_local
    width = master.shape[0]
    blocks = tokens // TOKEN_BLOCK + BLOCKS_PER_STEP
    step_rows = BLOCKS_PER_STEP * TOKEN_BLOCK
    core_pairs = [(i, i ^ 1) for i in range(rep_count)]
    chip_pairs = [(i, i ^ 2) for i in range(rep_count)]

    def table():
        return [pltpu.SMEM((blocks,), jnp.int32)] * 3

    def buffers(rows, columns):
        return pltpu.VMEM((BUFFERS, rows, columns), bf16)

    sems = pltpu.SemaphoreType.DMA((BUFFERS,))
    piece = (wide_count, 2, lines, width)
    for_core, weighted, near, far = pl.pallas_call(
        functools.partial(first_kernel, span, width, wide_count, rep_count),
        out_shape=(
            shape((cols, width), bf16),
            shape((cols, tokens), bf16),
            shape(piece, bf16),
            shape(piece, bf16),
        ),
        in_specs=[SMEM, HBM, HBM, VMEM],
        out_specs=(VMEM, HBM, VMEM, VMEM),
        scratch_shapes=table()
        + [
            buffers(step_rows, width),
            buffers(step_rows, cols),
            buffers(cols, step_rows),
            pltpu.VMEM((cols, width), f32),
            pltpu.VMEM((lines, hidden.shape[2]), f32),
            sems,
            sems,
            sems,
        ],
        compiler_params=PARAMS,
        name="first_chunk",
    )(seq_lengths, activations, value_grads, hidden)
    core_part = lax.ppermute(for_core, "rep", core_pairs)
    far_part = lax.ppermute(far, "rep", chip_pairs)

    def later(own_chip, taken, extra, out_shape):
        return pl.pallas_call(
            functools.partial(later_kernel, span, width, own_chip),
            out_shape=out_shape,
            in_specs=[SMEM, HBM, HBM] + [VMEM] * len(extra),
            out_specs=(VMEM,) * len(out_shape),
            scratch_shapes=table()
            + [
                buffers(step_rows, taken),
                buffers(cols, step_rows),
                pltpu.VMEM((cols, taken), f32),
                sems,
                sems,
            ],
            compiler_params=PARAMS,
            name="own_chunk" if own_chip else "second_chunk",
        )(seq_lengths, activations, weighted, *extra)

    (for_chip,) = later(False, width, (core_part,), (shape((cols, width), bf16),))
    chip_part = lax.ppermute(for_chip, "rep", chip_pairs)

    pieces = [jnp.stack([near[0], far_part[0]])]
    for dz in range(1, wide_count):
        pairs = [(i, i ^ dz) for i in range(wide_count)]
        pieces.append(lax.ppermute(jnp.stack([near[dz], far_part[dz]]), "wide", pairs))
    gathered = jnp.stack(pieces, axis=1)
    group_rows = 2 * wide_count * lines
    hidden_kept = gathered[:, :, 0].reshape(group_rows, width)
    hidden_sent = lax.ppermute(gathered[:, :, 1].reshape(group_rows, width), "rep", core_pairs)

    own_part, for_core = later(True, 2 * width, (), (shape((cols, width), f32), shape((cols, width), bf16)))
    core_part = lax.ppermute(for_core, "rep", core_pairs)

    kv_local = cols // HEAD
    rows = (HEADS // KV_HEADS) * lines
    mixed, late = pl.pallas_call(
        attention_kernel,
        out_shape=(shape((kv_local, rows, HEAD), f32), shape((kv_local, rows, lines), bf16)),
        in_specs=[SMEM, VMEM, VMEM, VMEM, VMEM, HBM],
        out_specs=(VMEM, VMEM),
        scratch_shapes=[pltpu.VMEM((lines, queries.shape[2]), f32), pltpu.VMEM((lines, cols), f32)],
        compiler_params=PARAMS,
        name="cache_attention",
    )(cache_lengths, queries, new_keys, cache_keys, cache_values, own_part)

    turned_spec = pl.BlockSpec((QUANT, width), lambda tile: (tile, 0))
    tile_spec = pl.BlockSpec((width, QUANT), lambda tile: (0, tile))
    hidden_spec = pl.BlockSpec((group_rows, width), lambda tile: (0, 0))
    part_spec = pl.BlockSpec((group_rows, QUANT), lambda tile: (0, tile))
    new_master, new_first, new_second, kept, sent = pl.pallas_call(
        update_kernel,
        grid=(cols // QUANT,),
        out_shape=(shape((width, cols), f32),) * 3
        + (shape((group_rows, cols), f32), shape((group_rows, cols), bf16)),
        in_specs=[turned_spec] * 3 + [tile_spec] * 3 + [hidden_spec] * 2,
        out_specs=(tile_spec,) * 3 + (part_spec,) * 2,
        compiler_params=PARAMS,
        name="update",
    )(own_part, core_part, chip_part, master, first_moment, second_moment, hidden_kept, hidden_sent)
    summed = kept + lax.ppermute(sent, "rep", core_pairs).astype(f32)
    half = wide_count * lines
    summed = summed[:half] + lax.ppermute(summed[half:].astype(bf16), "rep", chip_pairs).astype(f32)
    arrived = []
    for dz in range(1, wide_count):
        pairs = [(i, i ^ dz) for i in range(wide_count)]
        arrived.append(lax.ppermute(summed[dz * lines : (dz + 1) * lines].astype(bf16), "wide", pairs))
    new_values, attended = pl.pallas_call(
        functools.partial(finish_kernel, step_count, row_local),
        out_shape=(shape(new_keys.shape, bf16), shape(queries.shape, bf16)),
        in_specs=[VMEM] * (3 + len(arrived)),
        out_specs=(VMEM, VMEM),
        scratch_shapes=[pltpu.VMEM((lines, queries.shape[2]), f32)],
        compiler_params=PARAMS,
        name="finish",
    )(mixed, late, summed[:lines], *arrived)
    return (new_master, new_first, new_second, new_values, attended)


def dispatch(*args):
    activations, value_grads, seq_lengths, master, _, _, hidden = args[:7]
    lines = hidden.shape[0] * hidden.shape[1]
    wide_count = lax.axis_size("wide")
    fits = (
        lax.axis_size("rep") == 4
        and wide_count & (wide_count - 1) == 0
        and master.shape[0] % 128 == 0
        and master.shape[1] % QUANT == 0
        and (value_grads.shape[0] // seq_lengths.shape[0]) % TOKEN_BLOCK == 0
        and lines == 16
    )
    return (on_device if fits else on_device_plain)(*args)


def solution(mesh):
    in_specs = (
        P("rep", "wide"),
        P("rep", "tp"),
        P("rep"),
        P(("wide", "rep"), "tp"),
        P(("wide", "rep"), "tp"),
        P(("wide", "rep"), "tp"),
        P(None, ("wide", "rep"), None),
        P(None, ("wide", "rep"), "tp"),
        P(None, ("wide", "rep"), "tp"),
        P(("wide", "rep"), None, "tp"),
        P(("wide", "rep"), None, "tp"),
        P(("wide", "rep")),
    )
    out_specs = (
        P(("wide", "rep"), "tp"),
        P(("wide", "rep"), "tp"),
        P(("wide", "rep"), "tp"),
        P(None, ("wide", "rep"), "tp"),
        P(None, ("wide", "rep"), "tp"),
    )
    return jax.shard_map(
        dispatch, mesh=mesh, in_specs=in_specs, out_specs=out_specs, check_vma=False
    )
```

```python
import functools

import jax
import jax.numpy as jnp
from jax import lax
from jax.experimental import pallas as pl
from jax.experimental.pallas import tpu as pltpu
from jax.sharding import PartitionSpec as P


HEADS = 64
KV_HEADS = 8
HEAD = 128
QUANT = 128


beta_one = 0.9
beta_two = 0.95
learn_rate = 0.001
weight_decay = 0.1
epsilon = 1e-08
steps_done = 10.0
quant_top = 448.0
scale_epsilon = 1e-06


def quantize(weights):
    row_count, col_count = weights.shape
    tiled = weights.reshape(row_count, col_count // QUANT, QUANT)
    largest = jnp.max(jnp.abs(tiled), axis=2)
    scales = ((largest + scale_epsilon) / quant_top).astype(jnp.bfloat16)
    quantized = (tiled / scales.astype(jnp.float32)[:, :, None]).astype(jnp.bfloat16)
    return (quantized.reshape(row_count, col_count), scales)


def dequantize(quantized, scales):
    row_count, col_count = quantized.shape
    tiled = quantized.astype(jnp.float32).reshape(row_count, col_count // QUANT, QUANT)
    return (tiled * scales.astype(jnp.float32)[:, :, None]).reshape(row_count, col_count)


def on_device_plain(
    activations,
    value_grads,
    seq_lengths,
    master,
    first_moment,
    second_moment,
    hidden,
    queries,
    new_keys,
    cache_keys,
    cache_values,
    cache_lengths,
):
    seq_count = seq_lengths.shape[0]
    token_count, col_count = value_grads.shape
    seq_span = token_count // seq_count
    position = jnp.arange(seq_span, dtype=jnp.int32)
    lengths = seq_lengths.astype(jnp.float32)
    token_weight = jnp.where(position[None, :] < seq_lengths[:, None], 1.0 / lengths[:, None], 0.0)
    weighted = (
        value_grads.astype(jnp.float32).reshape(seq_count, seq_span, col_count)
        * token_weight[:, :, None]
    ).astype(jnp.bfloat16)
    weighted = weighted.reshape(token_count, col_count)
    gradient = lax.psum_scatter(
        lax.dot_general(
            activations, weighted, (((0,), (0,)), ((), ())), preferred_element_type=jnp.float32
        ),
        "rep",
        scatter_dimension=0,
        tiled=True,
    )
    new_first = beta_one * first_moment + (1.0 - beta_one) * gradient
    new_second = beta_two * second_moment + (1.0 - beta_two) * gradient * gradient
    corrected_first = new_first / (1.0 - beta_one**steps_done)
    corrected_second = new_second / (1.0 - beta_two**steps_done)
    new_master = master - learn_rate * (
        corrected_first / (jnp.sqrt(corrected_second) + epsilon) + weight_decay * master
    )
    quantized, scales = quantize(new_master)
    step_count, row_local, width = hidden.shape
    score_scale = HEAD ** (-0.5)
    group = HEADS // KV_HEADS
    kv_local = col_count // HEAD
    query = queries.reshape(step_count, row_local, kv_local, group, HEAD)
    keys_cache = cache_keys.reshape(row_local, cache_keys.shape[1], kv_local, HEAD)
    values_cache = cache_values.reshape(row_local, cache_values.shape[1], kv_local, HEAD)
    keys_new = new_keys.reshape(step_count, row_local, kv_local, HEAD)
    slots = jnp.arange(cache_keys.shape[1], dtype=jnp.int32)
    cache_live = slots[None, :] < cache_lengths[:, None]
    scores_cache = (
        jnp.einsum("sbgrd,bjgd->sbgrj", query, keys_cache, preferred_element_type=jnp.float32)
        * score_scale
    )
    scores_cache = jnp.where(cache_live[None, :, None, None, :], scores_cache, -jnp.inf)
    scores_new = (
        jnp.einsum("sbgrd,tbgd->sbgrt", query, keys_new, preferred_element_type=jnp.float32)
        * score_scale
    )
    moments = jnp.arange(step_count, dtype=jnp.int32)
    earlier = moments[None, :] <= moments[:, None]
    scores_new = jnp.where(earlier[:, None, None, None, :], scores_new, -jnp.inf)
    highest = jnp.maximum(jnp.max(scores_cache, axis=4), jnp.max(scores_new, axis=4))
    exp_cache = jnp.exp(scores_cache - highest[..., None])
    exp_new = jnp.exp(scores_new - highest[..., None])
    totals = jnp.sum(exp_cache, axis=4) + jnp.sum(exp_new, axis=4)
    probs_cache = (exp_cache / totals[..., None]).astype(jnp.bfloat16)
    probs_new = (exp_new / totals[..., None]).astype(jnp.bfloat16)
    mixed_cache = jnp.einsum(
        "sbgrj,bjgd->sbgrd", probs_cache, values_cache, preferred_element_type=jnp.float32
    )
    wide_count = lax.axis_size("wide")
    rep_count = lax.axis_size("rep")
    block_rows = width // (wide_count * rep_count)
    arranged = hidden.reshape(step_count, row_local, wide_count, rep_count, block_rows)
    swapped = lax.all_to_all(arranged, "rep", split_axis=3, concat_axis=1, tiled=True)
    group_rows = rep_count * row_local
    flat_group = swapped.reshape(step_count * group_rows, wide_count * block_rows).astype(
        jnp.float32
    )
    quant_rows = lax.all_gather(quantized, "wide", axis=0, tiled=True)
    scale_rows = lax.all_gather(scales, "wide", axis=0, tiled=True)
    weight_rows = dequantize(quant_rows, scale_rows)
    partial_value = jnp.dot(
        flat_group, weight_rows, precision=lax.Precision.HIGHEST, preferred_element_type=jnp.float32
    )
    partial_value = partial_value.reshape(step_count, group_rows, col_count)
    projected = lax.psum_scatter(partial_value, "rep", scatter_dimension=1, tiled=True)
    new_values = projected.astype(jnp.bfloat16)
    values_new = new_values.reshape(step_count, row_local, kv_local, HEAD)
    mixed = mixed_cache + jnp.einsum(
        "sbgrt,tbgd->sbgrd", probs_new, values_new, preferred_element_type=jnp.float32
    )
    attended = mixed.astype(jnp.bfloat16).reshape(step_count, row_local, kv_local * group * HEAD)
    return (new_master, new_first, new_second, new_values, attended)


TOKEN_BLOCK = 256
STEP_BLOCKS = 2
BUFFERS = 4
PAD = 4 * STEP_BLOCKS


def live_blocks(lengths, block_of, span, limit_of=None, length_of=None, begin=None):
    count = jnp.int32(0)
    per_seq = span // TOKEN_BLOCK

    def note(place, block, limit, length):
        block_of[place] = block
        if limit_of is not None:
            limit_of[place] = limit
            length_of[place] = length

    for seq in range(lengths.shape[0]):
        length = lengths[seq]
        for part in range(per_seq):
            note(count, seq * per_seq + part, length - part * TOKEN_BLOCK, length)
            count = count + jnp.where(length > part * TOKEN_BLOCK, 1, 0)
        if begin is not None and seq % STEP_BLOCKS == STEP_BLOCKS - 1 and seq // STEP_BLOCKS < BUFFERS - 1:
            begin(jnp.int32(seq // STEP_BLOCKS))
    for pad in range(PAD):
        note(count + pad, 0, 0, 1)
    return lax.div(count + STEP_BLOCKS - 1, STEP_BLOCKS)


def start_acts(acts, buf, sem, block_of, step, column, parts):
    width = buf.shape[1]
    for part in range(parts):
        first = pl.multiple_of(block_of[step * STEP_BLOCKS + part] * TOKEN_BLOCK, TOKEN_BLOCK)
        pltpu.make_async_copy(
            acts.at[pl.ds(first, TOKEN_BLOCK), pl.ds(column, width)],
            buf.at[part * TOKEN_BLOCK : (part + 1) * TOKEN_BLOCK],
            sem,
        ).start()


def wait_acts(acts, buf, sem):
    rows, cols = buf.shape
    pltpu.make_async_copy(acts.at[pl.ds(0, rows), pl.ds(0, cols)], buf, sem).wait()


def product(left, right):
    return jnp.dot(left, right, preferred_element_type=jnp.float32)


def first_kernel(
    span,
    width,
    wide_count,
    rep_count,
    lengths,
    acts,
    grads,
    hidden,
    ours,
    theirs,
    weighted,
    pieces,
    ahead,
    block_of,
    limit_of,
    length_of,
    acts_buf,
    grads_buf,
    even,
    odd,
    acc,
    loaded,
    flat,
    acts_sem,
    grads_sem,
    hidden_sem,
    ahead_sem,
):
    rep = lax.axis_index("rep")
    here = lax.axis_index("wide")
    core = lax.rem(rep, 2)
    chip = lax.div(rep, 2)
    column = pl.multiple_of((1 - chip) * 2 * width, 2 * width)
    next_column = pl.multiple_of((chip * 2 + 1 - core) * width, width)
    step_rows = STEP_BLOCKS * TOKEN_BLOCK
    cols = grads.shape[1]
    fetch = pltpu.make_async_copy(hidden, loaded, hidden_sem)
    fetch.start()

    def start(step):
        slot = lax.rem(step, BUFFERS)
        start_acts(grads, grads_buf.at[slot], grads_sem.at[slot], block_of, step, 0, STEP_BLOCKS)
        start_acts(acts, acts_buf.at[slot], acts_sem.at[slot], block_of, step, column, STEP_BLOCKS)

    def turn(step, target):
        slot = lax.rem(step, BUFFERS)
        for part in range(STEP_BLOCKS):
            entry = step * STEP_BLOCKS + part
            rows = slice(part * TOKEN_BLOCK, (part + 1) * TOKEN_BLOCK)
            value = grads_buf[slot, rows, :].astype(jnp.float32)
            length = jnp.full((1, cols), length_of[entry], jnp.int32).astype(jnp.float32)
            position = lax.broadcasted_iota(jnp.int32, value.shape, 0)
            scaled = jnp.where(position < limit_of[entry], value * (1.0 / length), 0.0)
            turned = scaled.astype(jnp.bfloat16).T
            target[:, rows] = turned
            place = pl.multiple_of(step * step_rows + part * TOKEN_BLOCK, TOKEN_BLOCK)
            weighted[:, pl.ds(place, TOKEN_BLOCK)] = turned

    steps = live_blocks(lengths, block_of, span, limit_of, length_of, start)
    start_acts(acts, ahead, ahead_sem, block_of, 0, next_column, 4 * STEP_BLOCKS)
    acc[...] = jnp.zeros_like(acc)
    fetch.wait()
    count, rows, _ = loaded.shape
    for step in range(count):
        flat[step * rows : (step + 1) * rows, :] = loaded[step].astype(jnp.float32)
    for dc in range(2):
        for dx in range(2):
            for dz in range(wide_count):
                place = (here ^ dz) * rep_count + (chip ^ dx) * 2 + (core ^ dc)
                begin = pl.multiple_of(place * width, width)
                pieces[dc * 2 + dx, dz] = flat[:, pl.ds(begin, width)].astype(jnp.bfloat16)

    wait_acts(grads, grads_buf.at[0], grads_sem.at[0])
    turn(jnp.int32(0), even)

    def phase(step, source, target):
        @pl.when(step + BUFFERS - 1 < steps)
        def _():
            start(step + BUFFERS - 1)

        @pl.when(step + 1 < steps)
        def _():
            slot = lax.rem(step + 1, BUFFERS)
            wait_acts(grads, grads_buf.at[slot], grads_sem.at[slot])

        slot = lax.rem(step, BUFFERS)
        wait_acts(acts, acts_buf.at[slot], acts_sem.at[slot])
        turn(step + 1, target)
        acc[...] += product(source[...], acts_buf[slot])

    def body(pair, carry):
        phase(2 * pair, even, odd)
        phase(2 * pair + 1, odd, even)
        return carry

    lax.fori_loop(0, lax.div(steps, 2), body, 0)

    @pl.when(lax.rem(steps, 2) == 1)
    def _():
        slot = lax.rem(steps - 1, BUFFERS)
        wait_acts(acts, acts_buf.at[slot], acts_sem.at[slot])
        acc[...] += product(even[...], acts_buf[slot])

    split(acc, core, ours, theirs)
    wait_acts(acts, ahead, ahead_sem)


def split(acc, core, ours, theirs):
    width = ours.shape[1]
    ours[...] = acc[:, pl.ds(pl.multiple_of(core * width, width), width)]
    theirs[...] = acc[:, pl.ds(pl.multiple_of((1 - core) * width, width), width)].astype(jnp.bfloat16)


def own_kernel(
    span,
    width,
    mine,
    lengths,
    acts,
    weighted,
    loaded,
    order,
    *refs,
):
    del order
    if mine:
        out, block_of, acts_buf, acc, acts_sem = refs
    else:
        out, ahead, block_of, acts_buf, acc, acts_sem, ahead_sem = refs
    rep = lax.axis_index("rep")
    core = lax.rem(rep, 2)
    first_column = lax.div(rep, 2) * 2 * width
    my_column = pl.multiple_of(first_column + core * width, width)
    column = my_column if mine else pl.multiple_of(first_column + (1 - core) * width, width)
    steps = live_blocks(lengths, block_of, span)
    trips = lax.div(steps, 4)
    rest = lax.rem(steps, 4)
    step_rows = STEP_BLOCKS * TOKEN_BLOCK
    trip_rows = 4 * step_rows
    slots = acts_buf.shape[0]
    held = trips + jnp.where(rest > 0, 1, 0)

    def start(trip):
        slot = lax.rem(trip, slots)
        start_acts(
            acts, acts_buf.at[slot], acts_sem.at[slot], block_of, 4 * trip, column, 4 * STEP_BLOCKS
        )

    for early in range(1, slots):
        @pl.when(early < held)
        def _():
            start(jnp.int32(early))

    if not mine:
        start_acts(acts, ahead, ahead_sem, block_of, 0, my_column, 4 * STEP_BLOCKS)
    acc[...] = product(weighted[:, :trip_rows], loaded[...])

    def body(trip, carry):
        @pl.when(trip + slots - 1 < held)
        def _():
            start(trip + slots - 1)

        slot = lax.rem(trip, slots)
        wait_acts(acts, acts_buf.at[slot], acts_sem.at[slot])
        lanes = pl.ds(pl.multiple_of(trip * trip_rows, trip_rows), trip_rows)
        acc[...] += product(weighted[:, lanes], acts_buf[slot])
        return carry

    lax.fori_loop(1, trips, body, 0)
    slot = lax.rem(trips, slots)
    begin = trips * trip_rows

    @pl.when(rest > 0)
    def _():
        wait_acts(acts, acts_buf.at[slot], acts_sem.at[slot])

    @pl.when(rest > 1)
    def _():
        lanes = pl.ds(pl.multiple_of(begin, trip_rows), 2 * step_rows)
        acc[...] += product(weighted[:, lanes], acts_buf[slot, : 2 * step_rows])

    @pl.when(lax.rem(rest, 2) == 1)
    def _():
        skipped = pl.multiple_of((rest - 1) * step_rows, 2 * step_rows)
        lanes = pl.ds(pl.multiple_of(begin + skipped, 2 * step_rows), step_rows)
        acc[...] += product(weighted[:, lanes], acts_buf[slot, pl.ds(skipped, step_rows)])

    out[...] = acc[...].astype(out.dtype)
    if not mine:
        wait_acts(acts, ahead, ahead_sem)


def update_kernel(
    own, from_core, from_chip, master, first, second, kept, sent,
    new_master, new_first, new_second, partial_kept, partial_sent,
):
    for tile in range(own.shape[0] // QUANT):
        part = slice(tile * QUANT, (tile + 1) * QUANT)
        total = own[part] + from_core[part].astype(jnp.float32) + from_chip[part].astype(jnp.float32)
        gradient = total.T
        moved_first = beta_one * first[:, part] + (1.0 - beta_one) * gradient
        moved_second = beta_two * second[:, part] + (1.0 - beta_two) * gradient * gradient
        corrected_first = moved_first * (learn_rate / (1.0 - beta_one**steps_done))
        corrected_second = moved_second * (1.0 / (1.0 - beta_two**steps_done))
        moved = master[:, part] * (1.0 - learn_rate * weight_decay) - corrected_first / (
            jnp.sqrt(corrected_second) + epsilon
        )
        new_first[:, part] = moved_first
        new_second[:, part] = moved_second
        new_master[:, part] = moved
        largest = jnp.max(jnp.abs(moved), axis=1, keepdims=True)
        scales = ((largest + scale_epsilon) / quant_top).astype(jnp.bfloat16).astype(jnp.float32)
        quantized = (moved * (1.0 / scales)).astype(jnp.bfloat16).astype(jnp.float32)
        used = quantized * scales
        high = used.astype(jnp.bfloat16)
        low = (used - high.astype(jnp.float32)).astype(jnp.bfloat16)
        partial_sent[:, part] = (product(sent[...], high) + product(sent[...], low)).astype(jnp.bfloat16)
        partial_kept[:, part] = product(kept[...], high) + product(kept[...], low)


def attention_kernel(
    lengths, queries, new_keys, cache_keys, cache_values, master, first, second,
    mixed, late, master_out, first_out, second_out, flat, keys, sems,
):
    writes = [
        pltpu.make_async_copy(source, target, sems.at[place])
        for place, (source, target) in enumerate(
            ((master, master_out), (first, first_out), (second, second_out))
        )
    ]
    for write in writes:
        write.start()
    steps, seqs, _ = queries.shape
    slots = cache_keys.shape[1]
    kv_local = new_keys.shape[2] // HEAD
    group = HEADS // KV_HEADS
    lines = steps * seqs
    for step in range(steps):
        flat[step * seqs : (step + 1) * seqs, :] = queries[step].astype(jnp.float32)
        keys[step * seqs : (step + 1) * seqs, :] = new_keys[step].astype(jnp.float32)
    rows = group * lines

    def index(shape, axis):
        return lax.broadcasted_iota(jnp.int32, shape, axis)

    wide_shape = (rows, slots)
    seq_of = lax.rem(index(wide_shape, 0), seqs)
    limit = jnp.zeros(wide_shape, jnp.int32)
    for seq in range(seqs):
        limit = jnp.where(seq_of == seq, lengths[seq], limit)
    live = index(wide_shape, 1) < limit
    late_shape = (rows, lines)
    late_row = index(late_shape, 0)
    late_col = index(late_shape, 1)
    allowed = (lax.rem(late_row, seqs) == lax.rem(late_col, seqs)) & (
        lax.div(late_col, seqs) <= lax.rem(lax.div(late_row, seqs), steps)
    )
    score_scale = HEAD ** (-0.5)
    across = (((1,), (1,)), ((), ()))
    for head in range(kv_local):
        lanes = slice(head * HEAD, (head + 1) * HEAD)
        query = jnp.concatenate(
            [
                flat[:, (head * group + part) * HEAD : (head * group + part + 1) * HEAD]
                for part in range(group)
            ],
            axis=0,
        ).astype(jnp.bfloat16)
        scores = jnp.zeros(wide_shape, jnp.float32)
        for seq in range(seqs):
            one = lax.dot_general(
                query, cache_keys[seq, :, lanes], across, preferred_element_type=jnp.float32
            )
            scores = jnp.where(seq_of == seq, one, scores)
        scores = jnp.where(live, scores * score_scale, -jnp.inf)
        scores_new = (
            lax.dot_general(
                query, keys[:, lanes].astype(jnp.bfloat16), across, preferred_element_type=jnp.float32
            )
            * score_scale
        )
        scores_new = jnp.where(allowed, scores_new, -jnp.inf)
        highest = jnp.maximum(
            jnp.max(scores, axis=1, keepdims=True), jnp.max(scores_new, axis=1, keepdims=True)
        )
        exp_cache = jnp.exp(scores - highest)
        exp_new = jnp.exp(scores_new - highest)
        totals = jnp.sum(exp_cache, axis=1, keepdims=True) + jnp.sum(exp_new, axis=1, keepdims=True)
        probs = exp_cache / totals
        late[head] = (exp_new / totals).astype(jnp.bfloat16)
        result = jnp.zeros((rows, HEAD), jnp.float32)
        for seq in range(seqs):
            mine = jnp.where(seq_of == seq, probs, 0.0).astype(jnp.bfloat16)
            result = result + jnp.dot(
                mine, cache_values[seq, :, lanes], preferred_element_type=jnp.float32
            )
        mixed[head] = result
    for write in writes:
        write.wait()


def finish_kernel(steps, seqs, *refs):
    mixed, late, own = refs[:3]
    arrived = refs[3:-3]
    new_values, attended, flat = refs[-3:]
    total = own[...]
    for block in arrived:
        total = total + block[...].astype(jnp.float32)
    values = total.astype(jnp.bfloat16)
    wide_values = values.astype(jnp.float32)
    lines = steps * seqs
    kv_local, rows, _ = mixed.shape
    group = rows // lines
    for head in range(kv_local):
        lanes = slice(head * HEAD, (head + 1) * HEAD)
        result = mixed[head] + jnp.dot(late[head], values[:, lanes], preferred_element_type=jnp.float32)
        for part in range(group):
            flat[:, (head * group + part) * HEAD : (head * group + part + 1) * HEAD] = result[
                part * lines : (part + 1) * lines, :
            ]
    for step in range(steps):
        new_values[step] = wide_values[step * seqs : (step + 1) * seqs, :].astype(jnp.bfloat16)
        attended[step] = flat[step * seqs : (step + 1) * seqs, :].astype(jnp.bfloat16)


HBM = pl.BlockSpec(memory_space=pltpu.HBM)
VMEM = pl.BlockSpec(memory_space=pltpu.VMEM)
SMEM = pl.BlockSpec(memory_space=pltpu.SMEM)
PARAMS = pltpu.CompilerParams(vmem_limit_bytes=24 * 1024 * 1024)


def on_device(
    activations,
    value_grads,
    seq_lengths,
    master,
    first_moment,
    second_moment,
    hidden,
    queries,
    new_keys,
    cache_keys,
    cache_values,
    cache_lengths,
):
    shape = jax.ShapeDtypeStruct
    bf16, f32 = jnp.bfloat16, jnp.float32
    wide_count = lax.axis_size("wide")
    rep_count = lax.axis_size("rep")
    tokens, cols = value_grads.shape
    seqs = seq_lengths.shape[0]
    span = tokens // seqs
    step_count, row_local, _ = hidden.shape
    lines = step_count * row_local
    width = master.shape[0]
    blocks = tokens // TOKEN_BLOCK + PAD
    step_rows = STEP_BLOCKS * TOKEN_BLOCK

    core_pairs = [(i, i ^ 1) for i in range(rep_count)]
    chip_pairs = [(i, i ^ 2) for i in range(rep_count)]

    table = pltpu.SMEM((blocks,), jnp.int32)

    def buffers(rows, columns):
        return pltpu.VMEM((BUFFERS, rows, columns), bf16)

    sems = pltpu.SemaphoreType.DMA((BUFFERS,))
    ours, for_core, weighted, pieces, ahead = pl.pallas_call(
        functools.partial(first_kernel, span, width, wide_count, rep_count),
        out_shape=(
            shape((cols, width), f32),
            shape((cols, width), bf16),
            pltpu.VMEM((cols, tokens + step_rows), bf16),
            shape((4, wide_count, lines, width), bf16),
            pltpu.VMEM((4 * step_rows, width), bf16),
        ),
        in_specs=[SMEM, HBM, HBM, HBM],
        out_specs=(VMEM,) * 5,
        scratch_shapes=[
            table,
            table,
            table,
            buffers(step_rows, 2 * width),
            buffers(step_rows, cols),
            pltpu.VMEM((cols, step_rows), bf16),
            pltpu.VMEM((cols, step_rows), bf16),
            pltpu.VMEM((cols, 2 * width), f32),
            pltpu.VMEM(hidden.shape, bf16),
            pltpu.VMEM((lines, hidden.shape[2]), f32),
            sems,
            sems,
            pltpu.SemaphoreType.DMA,
            pltpu.SemaphoreType.DMA,
        ],
        compiler_params=PARAMS,
        name="first_chunk",
    )(seq_lengths, activations, in_hbm(value_grads), in_hbm(hidden))
    core_part = lax.ppermute(for_core, "rep", core_pairs)
    both_pairs = [(i, i ^ 3) for i in range(rep_count)]
    moved = jnp.stack(
        [
            pieces[0],
            lax.ppermute(pieces[1], "rep", chip_pairs),
            lax.ppermute(pieces[2], "rep", core_pairs),
            lax.ppermute(pieces[3], "rep", both_pairs),
        ]
    )

    for_chip = (ours + core_part.astype(f32)).astype(bf16)
    chip_part = lax.ppermute(for_chip, "rep", chip_pairs)

    def own_call(mine, ahead, order, out_shape):
        return pl.pallas_call(
            functools.partial(own_kernel, span, width, mine),
            out_shape=out_shape,
            in_specs=[SMEM, HBM, VMEM, VMEM, HBM],
            out_specs=(VMEM,) * len(out_shape),
            scratch_shapes=[
                table,
                pltpu.VMEM((BUFFERS - 1, 4 * step_rows, width), bf16),
                pltpu.VMEM((cols, width), f32),
                pltpu.SemaphoreType.DMA((BUFFERS - 1,)),
            ]
            + [pltpu.SemaphoreType.DMA] * (not mine),
            compiler_params=PARAMS,
            name="own_chunk" if mine else "near_chunk",
        )(seq_lengths, activations, weighted, ahead, order)

    for_core, ahead = own_call(
        False, ahead, for_chip, (shape((cols, width), bf16), pltpu.VMEM((4 * step_rows, width), bf16))
    )
    core_part = lax.ppermute(for_core, "rep", core_pairs)
    pieces = [moved[:, 0]]
    for dz in range(1, wide_count):
        pairs = [(i, i ^ dz) for i in range(wide_count)]
        pieces.append(lax.ppermute(moved[:, dz], "wide", pairs))
    moved = jnp.stack(pieces, axis=1)
    group_rows = 2 * wide_count * lines
    hidden_kept = moved[:2].reshape(group_rows, width)
    hidden_sent = moved[2:].reshape(group_rows, width)

    (own_part,) = own_call(True, ahead, for_core, (shape((cols, width), f32),))
    new_master, new_first, new_second, kept, sent = pl.pallas_call(
        update_kernel,
        out_shape=(pltpu.VMEM((width, cols), f32),) * 3
        + (shape((group_rows, cols), f32), shape((group_rows, cols), bf16)),
        in_specs=[VMEM] * 8,
        out_specs=(VMEM,) * 5,
        compiler_params=PARAMS,
        name="update",
    )(own_part, core_part, chip_part, master, first_moment, second_moment, hidden_kept, hidden_sent)
    summed = kept + lax.ppermute(sent, "rep", core_pairs).astype(f32)
    half = wide_count * lines
    summed = summed[:half] + lax.ppermute(summed[half:].astype(bf16), "rep", chip_pairs).astype(f32)
    arrived = []
    for place in range(1, wide_count):
        pairs = [(i, i ^ place) for i in range(wide_count)]
        arrived.append(
            lax.ppermute(summed[place * lines : (place + 1) * lines].astype(bf16), "wide", pairs)
        )
    kv_local = cols // HEAD
    rows = (HEADS // KV_HEADS) * lines
    mixed, late, new_master, new_first, new_second = pl.pallas_call(
        attention_kernel,
        out_shape=(
            shape((kv_local, rows, HEAD), f32),
            shape((kv_local, rows, lines), bf16),
            *(pltpu.HBM((width, cols), f32),) * 3,
        ),
        in_specs=[SMEM] + [VMEM] * 7,
        out_specs=(VMEM, VMEM, HBM, HBM, HBM),
        scratch_shapes=[
            pltpu.VMEM((lines, queries.shape[2]), f32),
            pltpu.VMEM((lines, cols), f32),
            pltpu.SemaphoreType.DMA((3,)),
        ],
        compiler_params=PARAMS,
        name="cache_attention",
    )(cache_lengths, queries, new_keys, cache_keys, cache_values, new_master, new_first, new_second)
    new_values, attended = pl.pallas_call(
        functools.partial(finish_kernel, step_count, row_local),
        out_shape=(shape(new_keys.shape, bf16), shape(queries.shape, bf16)),
        in_specs=[VMEM] * (3 + len(arrived)),
        out_specs=(VMEM, VMEM),
        scratch_shapes=[pltpu.VMEM((lines, queries.shape[2]), f32)],
        compiler_params=PARAMS,
        name="finish",
    )(mixed, late, summed[:lines], *arrived)
    return (new_master, new_first, new_second, new_values, attended)


def in_hbm(value):
    return pltpu.with_memory_space_constraint(value, pltpu.HBM)


def dispatch(*args):
    _, value_grads, seq_lengths, master, _, _, hidden = args[:7]
    lines = hidden.shape[0] * hidden.shape[1]
    wide_count = lax.axis_size("wide")
    fits = (
        lax.axis_size("rep") == 4
        and wide_count & (wide_count - 1) == 0
        and master.shape[0] % 128 == 0
        and master.shape[1] % QUANT == 0
        and (value_grads.shape[0] // seq_lengths.shape[0]) % TOKEN_BLOCK == 0
        and lines == 16
        and seq_lengths.shape[0] >= BUFFERS * STEP_BLOCKS
    )
    if not fits:
        return on_device_plain(*args)
    return on_device(*args)


def solution(mesh):
    in_specs = (
        P("rep", "wide"),
        P("rep", "tp"),
        P("rep"),
        P(("wide", "rep"), "tp"),
        P(("wide", "rep"), "tp"),
        P(("wide", "rep"), "tp"),
        P(None, ("wide", "rep"), None),
        P(None, ("wide", "rep"), "tp"),
        P(None, ("wide", "rep"), "tp"),
        P(("wide", "rep"), None, "tp"),
        P(("wide", "rep"), None, "tp"),
        P(("wide", "rep")),
    )
    out_specs = (
        P(("wide", "rep"), "tp"),
        P(("wide", "rep"), "tp"),
        P(("wide", "rep"), "tp"),
        P(None, ("wide", "rep"), "tp"),
        P(None, ("wide", "rep"), "tp"),
    )
    return jax.shard_map(
        dispatch, mesh=mesh, in_specs=in_specs, out_specs=out_specs, check_vma=False
    )
```

```python
import functools

import jax
import jax.numpy as jnp
from jax import lax
from jax.experimental import pallas as pl
from jax.experimental.pallas import tpu as pltpu
from jax.sharding import PartitionSpec as P


HEADS = 64
KV_HEADS = 8
HEAD = 128
QUANT = 128


beta_one = 0.9
beta_two = 0.95
learn_rate = 0.001
weight_decay = 0.1
epsilon = 1e-08
steps_done = 10.0
quant_top = 448.0
scale_epsilon = 1e-06


def quantize(weights):
    row_count, col_count = weights.shape
    tiled = weights.reshape(row_count, col_count // QUANT, QUANT)
    largest = jnp.max(jnp.abs(tiled), axis=2)
    scales = ((largest + scale_epsilon) / quant_top).astype(jnp.bfloat16)
    quantized = (tiled / scales.astype(jnp.float32)[:, :, None]).astype(jnp.bfloat16)
    return (quantized.reshape(row_count, col_count), scales)


def dequantize(quantized, scales):
    row_count, col_count = quantized.shape
    tiled = quantized.astype(jnp.float32).reshape(row_count, col_count // QUANT, QUANT)
    return (tiled * scales.astype(jnp.float32)[:, :, None]).reshape(row_count, col_count)


def on_device_plain(
    activations,
    value_grads,
    seq_lengths,
    master,
    first_moment,
    second_moment,
    hidden,
    queries,
    new_keys,
    cache_keys,
    cache_values,
    cache_lengths,
):
    seq_count = seq_lengths.shape[0]
    token_count, col_count = value_grads.shape
    seq_span = token_count // seq_count
    position = jnp.arange(seq_span, dtype=jnp.int32)
    lengths = seq_lengths.astype(jnp.float32)
    token_weight = jnp.where(position[None, :] < seq_lengths[:, None], 1.0 / lengths[:, None], 0.0)
    weighted = (
        value_grads.astype(jnp.float32).reshape(seq_count, seq_span, col_count)
        * token_weight[:, :, None]
    ).astype(jnp.bfloat16)
    weighted = weighted.reshape(token_count, col_count)
    gradient = lax.psum_scatter(
        lax.dot_general(
            activations, weighted, (((0,), (0,)), ((), ())), preferred_element_type=jnp.float32
        ),
        "rep",
        scatter_dimension=0,
        tiled=True,
    )
    new_first = beta_one * first_moment + (1.0 - beta_one) * gradient
    new_second = beta_two * second_moment + (1.0 - beta_two) * gradient * gradient
    corrected_first = new_first / (1.0 - beta_one**steps_done)
    corrected_second = new_second / (1.0 - beta_two**steps_done)
    new_master = master - learn_rate * (
        corrected_first / (jnp.sqrt(corrected_second) + epsilon) + weight_decay * master
    )
    quantized, scales = quantize(new_master)
    step_count, row_local, width = hidden.shape
    score_scale = HEAD ** (-0.5)
    group = HEADS // KV_HEADS
    kv_local = col_count // HEAD
    query = queries.reshape(step_count, row_local, kv_local, group, HEAD)
    keys_cache = cache_keys.reshape(row_local, cache_keys.shape[1], kv_local, HEAD)
    values_cache = cache_values.reshape(row_local, cache_values.shape[1], kv_local, HEAD)
    keys_new = new_keys.reshape(step_count, row_local, kv_local, HEAD)
    slots = jnp.arange(cache_keys.shape[1], dtype=jnp.int32)
    cache_live = slots[None, :] < cache_lengths[:, None]
    scores_cache = (
        jnp.einsum("sbgrd,bjgd->sbgrj", query, keys_cache, preferred_element_type=jnp.float32)
        * score_scale
    )
    scores_cache = jnp.where(cache_live[None, :, None, None, :], scores_cache, -jnp.inf)
    scores_new = (
        jnp.einsum("sbgrd,tbgd->sbgrt", query, keys_new, preferred_element_type=jnp.float32)
        * score_scale
    )
    moments = jnp.arange(step_count, dtype=jnp.int32)
    earlier = moments[None, :] <= moments[:, None]
    scores_new = jnp.where(earlier[:, None, None, None, :], scores_new, -jnp.inf)
    highest = jnp.maximum(jnp.max(scores_cache, axis=4), jnp.max(scores_new, axis=4))
    exp_cache = jnp.exp(scores_cache - highest[..., None])
    exp_new = jnp.exp(scores_new - highest[..., None])
    totals = jnp.sum(exp_cache, axis=4) + jnp.sum(exp_new, axis=4)
    probs_cache = (exp_cache / totals[..., None]).astype(jnp.bfloat16)
    probs_new = (exp_new / totals[..., None]).astype(jnp.bfloat16)
    mixed_cache = jnp.einsum(
        "sbgrj,bjgd->sbgrd", probs_cache, values_cache, preferred_element_type=jnp.float32
    )
    wide_count = lax.axis_size("wide")
    rep_count = lax.axis_size("rep")
    block_rows = width // (wide_count * rep_count)
    arranged = hidden.reshape(step_count, row_local, wide_count, rep_count, block_rows)
    swapped = lax.all_to_all(arranged, "rep", split_axis=3, concat_axis=1, tiled=True)
    group_rows = rep_count * row_local
    flat_group = swapped.reshape(step_count * group_rows, wide_count * block_rows).astype(
        jnp.float32
    )
    quant_rows = lax.all_gather(quantized, "wide", axis=0, tiled=True)
    scale_rows = lax.all_gather(scales, "wide", axis=0, tiled=True)
    weight_rows = dequantize(quant_rows, scale_rows)
    partial_value = jnp.dot(
        flat_group, weight_rows, precision=lax.Precision.HIGHEST, preferred_element_type=jnp.float32
    )
    partial_value = partial_value.reshape(step_count, group_rows, col_count)
    projected = lax.psum_scatter(partial_value, "rep", scatter_dimension=1, tiled=True)
    new_values = projected.astype(jnp.bfloat16)
    values_new = new_values.reshape(step_count, row_local, kv_local, HEAD)
    mixed = mixed_cache + jnp.einsum(
        "sbgrt,tbgd->sbgrd", probs_new, values_new, preferred_element_type=jnp.float32
    )
    attended = mixed.astype(jnp.bfloat16).reshape(step_count, row_local, kv_local * group * HEAD)
    return (new_master, new_first, new_second, new_values, attended)


TOKEN_BLOCK = 128
STEP_BLOCKS = 4
BUFFERS = 5
TRIP_STEPS = 4
PAD = TRIP_STEPS * STEP_BLOCKS


def live_blocks(lengths, block_of, span, limit_of=None, length_of=None, begin=None):
    count = jnp.int32(0)
    per_seq = span // TOKEN_BLOCK

    def note(place, block, limit, length):
        block_of[place] = block
        if limit_of is not None:
            limit_of[place] = limit
            length_of[place] = length

    for seq in range(lengths.shape[0]):
        length = lengths[seq]
        for part in range(per_seq):
            note(count, seq * per_seq + part, length - part * TOKEN_BLOCK, length)
            count = count + jnp.where(length > part * TOKEN_BLOCK, 1, 0)
        if begin is not None and seq % STEP_BLOCKS == STEP_BLOCKS - 1 and seq // STEP_BLOCKS < BUFFERS - 1:
            begin(seq // STEP_BLOCKS)
    for pad in range(PAD):
        note(count + pad, 0, 0, 1)
    return jnp.maximum(lax.div(count + STEP_BLOCKS - 1, STEP_BLOCKS), TRIP_STEPS)


def start_acts(acts, buf, sem, block_of, step, column, parts, skip=0):
    width = buf.shape[1]
    for part in range(skip, parts):
        first = pl.multiple_of(block_of[step * STEP_BLOCKS + part] * TOKEN_BLOCK, TOKEN_BLOCK)
        pltpu.make_async_copy(
            acts.at[pl.ds(first, TOKEN_BLOCK), pl.ds(column, width)],
            buf.at[part * TOKEN_BLOCK : (part + 1) * TOKEN_BLOCK],
            sem,
        ).start()


def wait_acts(acts, buf, sem):
    rows, cols = buf.shape
    pltpu.make_async_copy(acts.at[pl.ds(0, rows), pl.ds(0, cols)], buf, sem).wait()


def product(left, right):
    return jnp.dot(left, right, preferred_element_type=jnp.float32)


def first_kernel(
    span,
    width,
    wide_count,
    rep_count,
    lengths_in,
    acts,
    grads,
    hidden,
    ours,
    theirs,
    weighted,
    pieces,
    ahead,
    lengths,
    block_of,
    limit_of,
    length_of,
    acts_buf,
    grads_buf,
    even,
    odd,
    acc,
    loaded,
    flat,
    acts_sem,
    grads_sem,
    hidden_sem,
    lengths_sem,
    ahead_sem,
):
    rep = lax.axis_index("rep")
    here = lax.axis_index("wide")
    core = lax.rem(rep, 2)
    chip = lax.div(rep, 2)
    column = pl.multiple_of((1 - chip) * 2 * width, 2 * width)
    next_column = pl.multiple_of((chip * 2 + 1 - core) * width, width)
    step_rows = STEP_BLOCKS * TOKEN_BLOCK
    cols = grads.shape[1]
    fetch_lengths = pltpu.make_async_copy(lengths_in, lengths, lengths_sem)
    fetch_lengths.start()
    for source, buf, sem, begin in ((grads, grads_buf, grads_sem, 0), (acts, acts_buf, acts_sem, column)):
        pltpu.make_async_copy(
            source.at[pl.ds(0, TOKEN_BLOCK), pl.ds(begin, buf.shape[2])],
            buf.at[0, :TOKEN_BLOCK],
            sem.at[0],
        ).start()
    fetch = pltpu.make_async_copy(hidden, loaded, hidden_sem)
    fetch.start()

    def start(step, skip=0):
        slot = lax.rem(step, BUFFERS)
        start_acts(grads, grads_buf.at[slot], grads_sem.at[slot], block_of, step, 0, STEP_BLOCKS, skip)
        start_acts(acts, acts_buf.at[slot], acts_sem.at[slot], block_of, step, column, STEP_BLOCKS, skip)

    def begin_step(step):
        start(jnp.int32(step), skip=1 if step == 0 else 0)

    def turn(step, target):
        slot = lax.rem(step, BUFFERS)
        for part in range(STEP_BLOCKS):
            entry = step * STEP_BLOCKS + part
            rows = slice(part * TOKEN_BLOCK, (part + 1) * TOKEN_BLOCK)
            value = grads_buf[slot, rows, :].astype(jnp.float32)
            length = jnp.full((1, cols), length_of[entry], jnp.int32).astype(jnp.float32)
            position = lax.broadcasted_iota(jnp.int32, value.shape, 0)
            scaled = jnp.where(position < limit_of[entry], value * (1.0 / length), 0.0)
            turned = scaled.astype(jnp.bfloat16).T
            target[:, rows] = turned
            place = pl.multiple_of(step * step_rows + part * TOKEN_BLOCK, TOKEN_BLOCK)
            weighted[:, pl.ds(place, TOKEN_BLOCK)] = turned

    acc[...] = jnp.zeros_like(acc)
    fetch_lengths.wait()
    steps = live_blocks(lengths, block_of, span, limit_of, length_of, begin_step)
    for early in range(lengths.shape[0] // STEP_BLOCKS, BUFFERS - 1):
        start(jnp.int32(early))
    fetch.wait()
    count, rows, _ = loaded.shape
    for step in range(count):
        flat[step * rows : (step + 1) * rows, :] = loaded[step].astype(jnp.float32)
    for dc in range(2):
        for dx in range(2):
            for dz in range(wide_count):
                place = (here ^ dz) * rep_count + (chip ^ dx) * 2 + (core ^ dc)
                begin = pl.multiple_of(place * width, width)
                pieces[dc * 2 + dx, dz] = flat[:, pl.ds(begin, width)].astype(jnp.bfloat16)

    wait_acts(grads, grads_buf.at[0], grads_sem.at[0])
    turn(jnp.int32(0), even)

    def phase(step, source, target):
        @pl.when(step + BUFFERS - 1 < steps)
        def _():
            start(step + BUFFERS - 1)

        @pl.when(step + 1 < steps)
        def _():
            slot = lax.rem(step + 1, BUFFERS)
            wait_acts(grads, grads_buf.at[slot], grads_sem.at[slot])

        slot = lax.rem(step, BUFFERS)
        wait_acts(acts, acts_buf.at[slot], acts_sem.at[slot])
        turn(step + 1, target)
        acc[...] += product(source[...], acts_buf[slot])

    def body(pair, carry):
        @pl.when(pair == 1)
        def _():
            start_acts(acts, ahead, ahead_sem, block_of, 0, next_column, 4 * STEP_BLOCKS)

        phase(2 * pair, even, odd)
        phase(2 * pair + 1, odd, even)
        return carry

    lax.fori_loop(0, lax.div(steps, 2), body, 0)

    @pl.when(lax.rem(steps, 2) == 1)
    def _():
        slot = lax.rem(steps - 1, BUFFERS)
        wait_acts(acts, acts_buf.at[slot], acts_sem.at[slot])
        acc[...] += product(even[...], acts_buf[slot])

    split(acc, core, ours, theirs)
    wait_acts(acts, ahead, ahead_sem)


def split(acc, core, ours, theirs):
    width = ours.shape[1]
    ours[...] = acc[:, pl.ds(pl.multiple_of(core * width, width), width)]
    theirs[...] = acc[:, pl.ds(pl.multiple_of((1 - core) * width, width), width)].astype(jnp.bfloat16)


def own_kernel(
    span,
    width,
    mine,
    lengths,
    acts,
    weighted,
    loaded,
    order,
    *refs,
):
    del order
    if mine:
        out, block_of, acts_buf, acc, acts_sem = refs
    else:
        out, ahead, block_of, acts_buf, acc, acts_sem, ahead_sem = refs
    rep = lax.axis_index("rep")
    core = lax.rem(rep, 2)
    first_column = lax.div(rep, 2) * 2 * width
    my_column = pl.multiple_of(first_column + core * width, width)
    column = my_column if mine else pl.multiple_of(first_column + (1 - core) * width, width)
    steps = live_blocks(lengths, block_of, span)
    trips = lax.div(steps, 4)
    rest = lax.rem(steps, 4)
    step_rows = STEP_BLOCKS * TOKEN_BLOCK
    trip_rows = 4 * step_rows
    slots = acts_buf.shape[0]
    held = trips + jnp.where(rest > 0, 1, 0)

    def start(trip):
        slot = lax.rem(trip, slots)
        start_acts(
            acts, acts_buf.at[slot], acts_sem.at[slot], block_of, 4 * trip, column, 4 * STEP_BLOCKS
        )

    for early in range(1, slots):
        @pl.when(early < held)
        def _():
            start(jnp.int32(early))

    acc[...] = product(weighted[:, :trip_rows], loaded[...])
    if not mine:
        start_acts(acts, ahead, ahead_sem, block_of, 0, my_column, 4 * STEP_BLOCKS)

    def body(trip, carry):
        @pl.when(trip + slots - 1 < held)
        def _():
            start(trip + slots - 1)

        slot = lax.rem(trip, slots)
        wait_acts(acts, acts_buf.at[slot], acts_sem.at[slot])
        lanes = pl.ds(pl.multiple_of(trip * trip_rows, trip_rows), trip_rows)
        acc[...] += product(weighted[:, lanes], acts_buf[slot])
        return carry

    lax.fori_loop(1, trips, body, 0)
    slot = lax.rem(trips, slots)
    begin = trips * trip_rows

    @pl.when(rest > 0)
    def _():
        wait_acts(acts, acts_buf.at[slot], acts_sem.at[slot])

    @pl.when(rest > 1)
    def _():
        lanes = pl.ds(pl.multiple_of(begin, trip_rows), 2 * step_rows)
        acc[...] += product(weighted[:, lanes], acts_buf[slot, : 2 * step_rows])

    @pl.when(lax.rem(rest, 2) == 1)
    def _():
        skipped = pl.multiple_of((rest - 1) * step_rows, 2 * step_rows)
        lanes = pl.ds(pl.multiple_of(begin + skipped, 2 * step_rows), step_rows)
        acc[...] += product(weighted[:, lanes], acts_buf[slot, pl.ds(skipped, step_rows)])

    out[...] = acc[...].astype(out.dtype)
    if not mine:
        wait_acts(acts, ahead, ahead_sem)


def update_kernel(
    own, from_core, from_chip, master, first, second, kept, sent,
    new_master, new_first, new_second, partial_kept, partial_sent,
):
    for tile in range(own.shape[0] // QUANT):
        part = slice(tile * QUANT, (tile + 1) * QUANT)
        total = own[part] + from_core[part].astype(jnp.float32) + from_chip[part].astype(jnp.float32)
        gradient = total.T
        moved_first = beta_one * first[:, part] + (1.0 - beta_one) * gradient
        moved_second = beta_two * second[:, part] + (1.0 - beta_two) * gradient * gradient
        corrected_first = moved_first * (learn_rate / (1.0 - beta_one**steps_done))
        corrected_second = moved_second * (1.0 / (1.0 - beta_two**steps_done))
        moved = master[:, part] * (1.0 - learn_rate * weight_decay) - corrected_first / (
            jnp.sqrt(corrected_second) + epsilon
        )
        new_first[:, part] = moved_first
        new_second[:, part] = moved_second
        new_master[:, part] = moved
        largest = jnp.max(jnp.abs(moved), axis=1, keepdims=True)
        scales = ((largest + scale_epsilon) / quant_top).astype(jnp.bfloat16).astype(jnp.float32)
        quantized = (moved * (1.0 / scales)).astype(jnp.bfloat16).astype(jnp.float32)
        used = quantized * scales
        high = used.astype(jnp.bfloat16)
        low = (used - high.astype(jnp.float32)).astype(jnp.bfloat16)
        partial_sent[:, part] = (product(sent[...], high) + product(sent[...], low)).astype(jnp.bfloat16)
        partial_kept[:, part] = product(kept[...], high) + product(kept[...], low)


def attention_kernel(
    lengths, queries, new_keys, cache_keys, cache_values, master, first, second,
    mixed, late, master_out, first_out, second_out, flat, keys, sems,
):
    writes = [
        pltpu.make_async_copy(source, target, sems.at[place])
        for place, (source, target) in enumerate(
            ((master, master_out), (first, first_out), (second, second_out))
        )
    ]
    for write in writes:
        write.start()
    steps, seqs, _ = queries.shape
    slots = cache_keys.shape[1]
    kv_local = new_keys.shape[2] // HEAD
    group = HEADS // KV_HEADS
    lines = steps * seqs
    for step in range(steps):
        flat[step * seqs : (step + 1) * seqs, :] = queries[step].astype(jnp.float32)
        keys[step * seqs : (step + 1) * seqs, :] = new_keys[step].astype(jnp.float32)
    rows = group * lines

    def index(shape, axis):
        return lax.broadcasted_iota(jnp.int32, shape, axis)

    wide_shape = (rows, slots)
    seq_of = lax.rem(index(wide_shape, 0), seqs)
    limit = jnp.zeros(wide_shape, jnp.int32)
    for seq in range(seqs):
        limit = jnp.where(seq_of == seq, lengths[seq], limit)
    live = index(wide_shape, 1) < limit
    late_shape = (rows, lines)
    late_row = index(late_shape, 0)
    late_col = index(late_shape, 1)
    allowed = (lax.rem(late_row, seqs) == lax.rem(late_col, seqs)) & (
        lax.div(late_col, seqs) <= lax.rem(lax.div(late_row, seqs), steps)
    )
    score_scale = HEAD ** (-0.5)
    across = (((1,), (1,)), ((), ()))
    for head in range(kv_local):
        lanes = slice(head * HEAD, (head + 1) * HEAD)
        query = jnp.concatenate(
            [
                flat[:, (head * group + part) * HEAD : (head * group + part + 1) * HEAD]
                for part in range(group)
            ],
            axis=0,
        ).astype(jnp.bfloat16)
        scores = jnp.zeros(wide_shape, jnp.float32)
        for seq in range(seqs):
            one = lax.dot_general(
                query, cache_keys[seq, :, lanes], across, preferred_element_type=jnp.float32
            )
            scores = jnp.where(seq_of == seq, one, scores)
        scores = jnp.where(live, scores * score_scale, -jnp.inf)
        scores_new = (
            lax.dot_general(
                query, keys[:, lanes].astype(jnp.bfloat16), across, preferred_element_type=jnp.float32
            )
            * score_scale
        )
        scores_new = jnp.where(allowed, scores_new, -jnp.inf)
        highest = jnp.maximum(
            jnp.max(scores, axis=1, keepdims=True), jnp.max(scores_new, axis=1, keepdims=True)
        )
        exp_cache = jnp.exp(scores - highest)
        exp_new = jnp.exp(scores_new - highest)
        totals = jnp.sum(exp_cache, axis=1, keepdims=True) + jnp.sum(exp_new, axis=1, keepdims=True)
        probs = exp_cache / totals
        late[head] = (exp_new / totals).astype(jnp.bfloat16)
        result = jnp.zeros((rows, HEAD), jnp.float32)
        for seq in range(seqs):
            mine = jnp.where(seq_of == seq, probs, 0.0).astype(jnp.bfloat16)
            result = result + jnp.dot(
                mine, cache_values[seq, :, lanes], preferred_element_type=jnp.float32
            )
        mixed[head] = result
    for write in writes:
        write.wait()


def finish_kernel(steps, seqs, *refs):
    mixed, late, own = refs[:3]
    arrived = refs[3:-3]
    new_values, attended, flat = refs[-3:]
    total = own[...]
    for block in arrived:
        total = total + block[...].astype(jnp.float32)
    values = total.astype(jnp.bfloat16)
    wide_values = values.astype(jnp.float32)
    lines = steps * seqs
    kv_local, rows, _ = mixed.shape
    group = rows // lines
    for head in range(kv_local):
        lanes = slice(head * HEAD, (head + 1) * HEAD)
        result = mixed[head] + jnp.dot(late[head], values[:, lanes], preferred_element_type=jnp.float32)
        for part in range(group):
            flat[:, (head * group + part) * HEAD : (head * group + part + 1) * HEAD] = result[
                part * lines : (part + 1) * lines, :
            ]
    for step in range(steps):
        new_values[step] = wide_values[step * seqs : (step + 1) * seqs, :].astype(jnp.bfloat16)
        attended[step] = flat[step * seqs : (step + 1) * seqs, :].astype(jnp.bfloat16)


HBM = pl.BlockSpec(memory_space=pltpu.HBM)
VMEM = pl.BlockSpec(memory_space=pltpu.VMEM)
SMEM = pl.BlockSpec(memory_space=pltpu.SMEM)
PARAMS = pltpu.CompilerParams(vmem_limit_bytes=24 * 1024 * 1024)


def on_device(
    activations,
    value_grads,
    seq_lengths,
    master,
    first_moment,
    second_moment,
    hidden,
    queries,
    new_keys,
    cache_keys,
    cache_values,
    cache_lengths,
):
    shape = jax.ShapeDtypeStruct
    bf16, f32 = jnp.bfloat16, jnp.float32
    wide_count = lax.axis_size("wide")
    rep_count = lax.axis_size("rep")
    tokens, cols = value_grads.shape
    seqs = seq_lengths.shape[0]
    span = tokens // seqs
    step_count, row_local, _ = hidden.shape
    lines = step_count * row_local
    width = master.shape[0]
    blocks = tokens // TOKEN_BLOCK + PAD
    step_rows = STEP_BLOCKS * TOKEN_BLOCK

    core_pairs = [(i, i ^ 1) for i in range(rep_count)]
    chip_pairs = [(i, i ^ 2) for i in range(rep_count)]

    table = pltpu.SMEM((blocks,), jnp.int32)

    def buffers(rows, columns):
        return pltpu.VMEM((BUFFERS, rows, columns), bf16)

    sems = pltpu.SemaphoreType.DMA((BUFFERS,))
    ours, for_core, weighted, pieces, ahead = pl.pallas_call(
        functools.partial(first_kernel, span, width, wide_count, rep_count),
        out_shape=(
            shape((cols, width), f32),
            shape((cols, width), bf16),
            pltpu.VMEM((cols, tokens + step_rows), bf16),
            shape((4, wide_count, lines, width), bf16),
            pltpu.VMEM((4 * step_rows, width), bf16),
        ),
        in_specs=[HBM, HBM, HBM, HBM],
        out_specs=(VMEM,) * 5,
        scratch_shapes=[
            pltpu.SMEM(seq_lengths.shape, jnp.int32),
            table,
            table,
            table,
            buffers(step_rows, 2 * width),
            buffers(step_rows, cols),
            pltpu.VMEM((cols, step_rows), bf16),
            pltpu.VMEM((cols, step_rows), bf16),
            pltpu.VMEM((cols, 2 * width), f32),
            pltpu.VMEM(hidden.shape, bf16),
            pltpu.VMEM((lines, hidden.shape[2]), f32),
            sems,
            sems,
            pltpu.SemaphoreType.DMA,
            pltpu.SemaphoreType.DMA,
            pltpu.SemaphoreType.DMA,
        ],
        compiler_params=PARAMS,
        name="first_chunk",
    )(in_hbm(seq_lengths), activations, in_hbm(value_grads), in_hbm(hidden))
    core_part = lax.ppermute(for_core, "rep", core_pairs)
    both_pairs = [(i, i ^ 3) for i in range(rep_count)]
    moved = jnp.stack(
        [
            pieces[0],
            lax.ppermute(pieces[1], "rep", chip_pairs),
            lax.ppermute(pieces[2], "rep", core_pairs),
            lax.ppermute(pieces[3], "rep", both_pairs),
        ]
    )

    for_chip = (ours + core_part.astype(f32)).astype(bf16)
    chip_part = lax.ppermute(for_chip, "rep", chip_pairs)

    def own_call(mine, ahead, order, out_shape):
        return pl.pallas_call(
            functools.partial(own_kernel, span, width, mine),
            out_shape=out_shape,
            in_specs=[SMEM, HBM, VMEM, VMEM, HBM],
            out_specs=(VMEM,) * len(out_shape),
            scratch_shapes=[
                table,
                pltpu.VMEM((3, 4 * step_rows, width), bf16),
                pltpu.VMEM((cols, width), f32),
                pltpu.SemaphoreType.DMA((3,)),
            ]
            + [pltpu.SemaphoreType.DMA] * (not mine),
            compiler_params=PARAMS,
            name="own_chunk" if mine else "near_chunk",
        )(seq_lengths, activations, weighted, ahead, order)

    for_core, ahead = own_call(
        False, ahead, for_chip, (shape((cols, width), bf16), pltpu.VMEM((4 * step_rows, width), bf16))
    )
    core_part = lax.ppermute(for_core, "rep", core_pairs)
    pieces = [moved[:, 0]]
    for dz in range(1, wide_count):
        pairs = [(i, i ^ dz) for i in range(wide_count)]
        pieces.append(lax.ppermute(moved[:, dz], "wide", pairs))
    moved = jnp.stack(pieces, axis=1)
    group_rows = 2 * wide_count * lines
    hidden_kept = moved[:2].reshape(group_rows, width)
    hidden_sent = moved[2:].reshape(group_rows, width)

    (own_part,) = own_call(True, ahead, for_core, (shape((cols, width), f32),))
    new_master, new_first, new_second, kept, sent = pl.pallas_call(
        update_kernel,
        out_shape=(pltpu.VMEM((width, cols), f32),) * 3
        + (shape((group_rows, cols), f32), shape((group_rows, cols), bf16)),
        in_specs=[VMEM] * 8,
        out_specs=(VMEM,) * 5,
        compiler_params=PARAMS,
        name="update",
    )(own_part, core_part, chip_part, master, first_moment, second_moment, hidden_kept, hidden_sent)
    summed = kept + lax.ppermute(sent, "rep", core_pairs).astype(f32)
    half = wide_count * lines
    summed = summed[:half] + lax.ppermute(summed[half:].astype(bf16), "rep", chip_pairs).astype(f32)
    arrived = []
    for place in range(1, wide_count):
        pairs = [(i, i ^ place) for i in range(wide_count)]
        arrived.append(
            lax.ppermute(summed[place * lines : (place + 1) * lines].astype(bf16), "wide", pairs)
        )
    kv_local = cols // HEAD
    rows = (HEADS // KV_HEADS) * lines
    mixed, late, new_master, new_first, new_second = pl.pallas_call(
        attention_kernel,
        out_shape=(
            shape((kv_local, rows, HEAD), f32),
            shape((kv_local, rows, lines), bf16),
            *(pltpu.HBM((width, cols), f32),) * 3,
        ),
        in_specs=[SMEM] + [VMEM] * 7,
        out_specs=(VMEM, VMEM, HBM, HBM, HBM),
        scratch_shapes=[
            pltpu.VMEM((lines, queries.shape[2]), f32),
            pltpu.VMEM((lines, cols), f32),
            pltpu.SemaphoreType.DMA((3,)),
        ],
        compiler_params=PARAMS,
        name="cache_attention",
    )(cache_lengths, queries, new_keys, cache_keys, cache_values, new_master, new_first, new_second)
    new_values, attended = pl.pallas_call(
        functools.partial(finish_kernel, step_count, row_local),
        out_shape=(shape(new_keys.shape, bf16), shape(queries.shape, bf16)),
        in_specs=[VMEM] * (3 + len(arrived)),
        out_specs=(VMEM, VMEM),
        scratch_shapes=[pltpu.VMEM((lines, queries.shape[2]), f32)],
        compiler_params=PARAMS,
        name="finish",
    )(mixed, late, summed[:lines], *arrived)
    return (new_master, new_first, new_second, new_values, attended)


def in_hbm(value):
    return pltpu.with_memory_space_constraint(value, pltpu.HBM)


def dispatch(*args):
    _, value_grads, seq_lengths, master, _, _, hidden = args[:7]
    lines = hidden.shape[0] * hidden.shape[1]
    wide_count = lax.axis_size("wide")
    fits = (
        lax.axis_size("rep") == 4
        and wide_count & (wide_count - 1) == 0
        and master.shape[0] % 128 == 0
        and master.shape[1] % QUANT == 0
        and (value_grads.shape[0] // seq_lengths.shape[0]) % TOKEN_BLOCK == 0
        and lines == 16
        and seq_lengths.shape[0] >= STEP_BLOCKS
    )
    if not fits:
        return on_device_plain(*args)
    return on_device(*args)


def solution(mesh):
    in_specs = (
        P("rep", "wide"),
        P("rep", "tp"),
        P("rep"),
        P(("wide", "rep"), "tp"),
        P(("wide", "rep"), "tp"),
        P(("wide", "rep"), "tp"),
        P(None, ("wide", "rep"), None),
        P(None, ("wide", "rep"), "tp"),
        P(None, ("wide", "rep"), "tp"),
        P(("wide", "rep"), None, "tp"),
        P(("wide", "rep"), None, "tp"),
        P(("wide", "rep")),
    )
    out_specs = (
        P(("wide", "rep"), "tp"),
        P(("wide", "rep"), "tp"),
        P(("wide", "rep"), "tp"),
        P(None, ("wide", "rep"), "tp"),
        P(None, ("wide", "rep"), "tp"),
    )
    return jax.shard_map(
        dispatch, mesh=mesh, in_specs=in_specs, out_specs=out_specs, check_vma=False
    )
```

```python
import functools

import jax
import jax.numpy as jnp
from jax import lax
from jax.experimental import pallas as pl
from jax.experimental.pallas import tpu as pltpu
from jax.sharding import PartitionSpec as P


HEADS = 64
KV_HEADS = 8
HEAD = 128
QUANT = 128


beta_one = 0.9
beta_two = 0.95
learn_rate = 0.001
weight_decay = 0.1
epsilon = 1e-08
steps_done = 10.0
quant_top = 448.0
scale_epsilon = 1e-06


def quantize(weights):
    row_count, col_count = weights.shape
    tiled = weights.reshape(row_count, col_count // QUANT, QUANT)
    largest = jnp.max(jnp.abs(tiled), axis=2)
    scales = ((largest + scale_epsilon) / quant_top).astype(jnp.bfloat16)
    quantized = (tiled / scales.astype(jnp.float32)[:, :, None]).astype(jnp.bfloat16)
    return (quantized.reshape(row_count, col_count), scales)


def dequantize(quantized, scales):
    row_count, col_count = quantized.shape
    tiled = quantized.astype(jnp.float32).reshape(row_count, col_count // QUANT, QUANT)
    return (tiled * scales.astype(jnp.float32)[:, :, None]).reshape(row_count, col_count)


def on_device_plain(
    activations,
    value_grads,
    seq_lengths,
    master,
    first_moment,
    second_moment,
    hidden,
    queries,
    new_keys,
    cache_keys,
    cache_values,
    cache_lengths,
):
    seq_count = seq_lengths.shape[0]
    token_count, col_count = value_grads.shape
    seq_span = token_count // seq_count
    position = jnp.arange(seq_span, dtype=jnp.int32)
    lengths = seq_lengths.astype(jnp.float32)
    token_weight = jnp.where(position[None, :] < seq_lengths[:, None], 1.0 / lengths[:, None], 0.0)
    weighted = (
        value_grads.astype(jnp.float32).reshape(seq_count, seq_span, col_count)
        * token_weight[:, :, None]
    ).astype(jnp.bfloat16)
    weighted = weighted.reshape(token_count, col_count)
    gradient = lax.psum_scatter(
        lax.dot_general(
            activations, weighted, (((0,), (0,)), ((), ())), preferred_element_type=jnp.float32
        ),
        "rep",
        scatter_dimension=0,
        tiled=True,
    )
    new_first = beta_one * first_moment + (1.0 - beta_one) * gradient
    new_second = beta_two * second_moment + (1.0 - beta_two) * gradient * gradient
    corrected_first = new_first / (1.0 - beta_one**steps_done)
    corrected_second = new_second / (1.0 - beta_two**steps_done)
    new_master = master - learn_rate * (
        corrected_first / (jnp.sqrt(corrected_second) + epsilon) + weight_decay * master
    )
    quantized, scales = quantize(new_master)
    step_count, row_local, width = hidden.shape
    score_scale = HEAD ** (-0.5)
    group = HEADS // KV_HEADS
    kv_local = col_count // HEAD
    query = queries.reshape(step_count, row_local, kv_local, group, HEAD)
    keys_cache = cache_keys.reshape(row_local, cache_keys.shape[1], kv_local, HEAD)
    values_cache = cache_values.reshape(row_local, cache_values.shape[1], kv_local, HEAD)
    keys_new = new_keys.reshape(step_count, row_local, kv_local, HEAD)
    slots = jnp.arange(cache_keys.shape[1], dtype=jnp.int32)
    cache_live = slots[None, :] < cache_lengths[:, None]
    scores_cache = (
        jnp.einsum("sbgrd,bjgd->sbgrj", query, keys_cache, preferred_element_type=jnp.float32)
        * score_scale
    )
    scores_cache = jnp.where(cache_live[None, :, None, None, :], scores_cache, -jnp.inf)
    scores_new = (
        jnp.einsum("sbgrd,tbgd->sbgrt", query, keys_new, preferred_element_type=jnp.float32)
        * score_scale
    )
    moments = jnp.arange(step_count, dtype=jnp.int32)
    earlier = moments[None, :] <= moments[:, None]
    scores_new = jnp.where(earlier[:, None, None, None, :], scores_new, -jnp.inf)
    highest = jnp.maximum(jnp.max(scores_cache, axis=4), jnp.max(scores_new, axis=4))
    exp_cache = jnp.exp(scores_cache - highest[..., None])
    exp_new = jnp.exp(scores_new - highest[..., None])
    totals = jnp.sum(exp_cache, axis=4) + jnp.sum(exp_new, axis=4)
    probs_cache = (exp_cache / totals[..., None]).astype(jnp.bfloat16)
    probs_new = (exp_new / totals[..., None]).astype(jnp.bfloat16)
    mixed_cache = jnp.einsum(
        "sbgrj,bjgd->sbgrd", probs_cache, values_cache, preferred_element_type=jnp.float32
    )
    wide_count = lax.axis_size("wide")
    rep_count = lax.axis_size("rep")
    block_rows = width // (wide_count * rep_count)
    arranged = hidden.reshape(step_count, row_local, wide_count, rep_count, block_rows)
    swapped = lax.all_to_all(arranged, "rep", split_axis=3, concat_axis=1, tiled=True)
    group_rows = rep_count * row_local
    flat_group = swapped.reshape(step_count * group_rows, wide_count * block_rows).astype(
        jnp.float32
    )
    quant_rows = lax.all_gather(quantized, "wide", axis=0, tiled=True)
    scale_rows = lax.all_gather(scales, "wide", axis=0, tiled=True)
    weight_rows = dequantize(quant_rows, scale_rows)
    partial_value = jnp.dot(
        flat_group, weight_rows, precision=lax.Precision.HIGHEST, preferred_element_type=jnp.float32
    )
    partial_value = partial_value.reshape(step_count, group_rows, col_count)
    projected = lax.psum_scatter(partial_value, "rep", scatter_dimension=1, tiled=True)
    new_values = projected.astype(jnp.bfloat16)
    values_new = new_values.reshape(step_count, row_local, kv_local, HEAD)
    mixed = mixed_cache + jnp.einsum(
        "sbgrt,tbgd->sbgrd", probs_new, values_new, preferred_element_type=jnp.float32
    )
    attended = mixed.astype(jnp.bfloat16).reshape(step_count, row_local, kv_local * group * HEAD)
    return (new_master, new_first, new_second, new_values, attended)


TOKEN_BLOCK = 128
STEP_BLOCKS = 4
BUFFERS = 7
TRIP_STEPS = 4
PAD = TRIP_STEPS * STEP_BLOCKS


def live_blocks(lengths, block_of, span, limit_of=None, length_of=None):
    per_seq = span // TOKEN_BLOCK
    seqs = lengths.shape[0]

    def note(place, block, limit, length):
        block_of[place] = block
        if limit_of is not None:
            limit_of[place] = limit
            length_of[place] = length

    for seq in range(seqs):
        note(seq, seq * per_seq, lengths[seq], lengths[seq])
    count = jnp.int32(seqs)
    for seq in range(seqs):
        length = lengths[seq]
        for part in range(1, per_seq):
            note(count, seq * per_seq + part, length - part * TOKEN_BLOCK, length)
            count = count + jnp.where(length > part * TOKEN_BLOCK, 1, 0)
    for pad in range(PAD):
        note(count + pad, 0, 0, 1)
    return jnp.maximum(lax.div(count + STEP_BLOCKS - 1, STEP_BLOCKS), TRIP_STEPS)


def start_acts(acts, buf, sem, block_of, step, column, parts):
    width = buf.shape[1]
    for part in range(parts):
        first = pl.multiple_of(block_of[step * STEP_BLOCKS + part] * TOKEN_BLOCK, TOKEN_BLOCK)
        pltpu.make_async_copy(
            acts.at[pl.ds(first, TOKEN_BLOCK), pl.ds(column, width)],
            buf.at[part * TOKEN_BLOCK : (part + 1) * TOKEN_BLOCK],
            sem,
        ).start()


def wait_acts(acts, buf, sem):
    rows, cols = buf.shape
    pltpu.make_async_copy(acts.at[pl.ds(0, rows), pl.ds(0, cols)], buf, sem).wait()


def start_ahead(acts, ahead, sem, block_of, steps, column):
    start_acts(acts, ahead.at[0], sem.at[0], block_of, 0, column, TRIP_STEPS * STEP_BLOCKS)

    @pl.when(steps >= 2 * TRIP_STEPS)
    def _():
        start_acts(
            acts, ahead.at[1], sem.at[1], block_of, TRIP_STEPS, column, TRIP_STEPS * STEP_BLOCKS
        )


def wait_ahead(acts, ahead, sem, steps):
    wait_acts(acts, ahead.at[0], sem.at[0])

    @pl.when(steps >= 2 * TRIP_STEPS)
    def _():
        wait_acts(acts, ahead.at[1], sem.at[1])


def product(left, right):
    return jnp.dot(left, right, preferred_element_type=jnp.float32)


def first_kernel(
    span,
    width,
    wide_count,
    rep_count,
    lengths_in,
    acts,
    grads,
    hidden,
    ours,
    theirs,
    weighted,
    pieces,
    ahead,
    lengths,
    block_of,
    limit_of,
    length_of,
    acts_buf,
    grads_buf,
    even,
    odd,
    acc,
    loaded,
    flat,
    acts_sem,
    grads_sem,
    hidden_sem,
    lengths_sem,
    ahead_sem,
):
    rep = lax.axis_index("rep")
    here = lax.axis_index("wide")
    core = lax.rem(rep, 2)
    chip = lax.div(rep, 2)
    column = pl.multiple_of((1 - chip) * 2 * width, 2 * width)
    next_column = pl.multiple_of((chip * 2 + 1 - core) * width, width)
    step_rows = STEP_BLOCKS * TOKEN_BLOCK
    cols = grads.shape[1]
    fetch_lengths = pltpu.make_async_copy(lengths_in, lengths, lengths_sem)
    fetch_lengths.start()

    def start(step, blocks=block_of):
        slot = step % BUFFERS if isinstance(step, int) else lax.rem(step, BUFFERS)
        start_acts(grads, grads_buf.at[slot], grads_sem.at[slot], blocks, step, 0, STEP_BLOCKS)
        start_acts(acts, acts_buf.at[slot], acts_sem.at[slot], blocks, step, column, STEP_BLOCKS)

    known = [seq * (span // TOKEN_BLOCK) for seq in range(lengths.shape[0])]
    known_steps = len(known) // STEP_BLOCKS
    start(0, known)
    fetch = pltpu.make_async_copy(hidden, loaded, hidden_sem)
    fetch.start()
    for early in range(1, known_steps):
        start(early, known)

    def turn(step, target):
        slot = lax.rem(step, BUFFERS)
        for part in range(STEP_BLOCKS):
            entry = step * STEP_BLOCKS + part
            rows = slice(part * TOKEN_BLOCK, (part + 1) * TOKEN_BLOCK)
            value = grads_buf[slot, rows, :].astype(jnp.float32)
            length = jnp.full((1, cols), length_of[entry], jnp.int32).astype(jnp.float32)
            position = lax.broadcasted_iota(jnp.int32, value.shape, 0)
            scaled = jnp.where(position < limit_of[entry], value * (1.0 / length), 0.0)
            turned = scaled.astype(jnp.bfloat16).T
            target[:, rows] = turned
            place = pl.multiple_of(step * step_rows + part * TOKEN_BLOCK, TOKEN_BLOCK)
            weighted[:, pl.ds(place, TOKEN_BLOCK)] = turned

    acc[...] = jnp.zeros_like(acc)
    fetch_lengths.wait()
    steps = live_blocks(lengths, block_of, span, limit_of, length_of)
    for early in range(known_steps, BUFFERS - 1):
        @pl.when(early < steps)
        def _():
            start(early)

    fetch.wait()
    count, rows, _ = loaded.shape
    for step in range(count):
        flat[step * rows : (step + 1) * rows, :] = loaded[step].astype(jnp.float32)
    for dc in range(2):
        for dx in range(2):
            for dz in range(wide_count):
                place = (here ^ dz) * rep_count + (chip ^ dx) * 2 + (core ^ dc)
                begin = pl.multiple_of(place * width, width)
                pieces[dc * 2 + dx, dz] = flat[:, pl.ds(begin, width)].astype(jnp.bfloat16)

    wait_acts(grads, grads_buf.at[0], grads_sem.at[0])
    turn(jnp.int32(0), even)

    def phase(step, source, target):
        @pl.when(step + BUFFERS - 1 < steps)
        def _():
            start(step + BUFFERS - 1)

        @pl.when(step + 1 < steps)
        def _():
            slot = lax.rem(step + 1, BUFFERS)
            wait_acts(grads, grads_buf.at[slot], grads_sem.at[slot])

        slot = lax.rem(step, BUFFERS)
        wait_acts(acts, acts_buf.at[slot], acts_sem.at[slot])
        turn(step + 1, target)
        acc[...] += product(source[...], acts_buf[slot])

    def body(pair, carry):
        @pl.when(pair == 1)
        def _():
            start_ahead(acts, ahead, ahead_sem, block_of, steps, next_column)

        phase(2 * pair, even, odd)
        phase(2 * pair + 1, odd, even)
        return carry

    lax.fori_loop(0, lax.div(steps, 2), body, 0)

    @pl.when(lax.rem(steps, 2) == 1)
    def _():
        slot = lax.rem(steps - 1, BUFFERS)
        wait_acts(acts, acts_buf.at[slot], acts_sem.at[slot])
        acc[...] += product(even[...], acts_buf[slot])

    split(acc, core, ours, theirs)
    wait_ahead(acts, ahead, ahead_sem, steps)


def split(acc, core, ours, theirs):
    width = ours.shape[1]
    ours[...] = acc[:, pl.ds(pl.multiple_of(core * width, width), width)]
    theirs[...] = acc[:, pl.ds(pl.multiple_of((1 - core) * width, width), width)].astype(jnp.bfloat16)


def own_kernel(
    span,
    width,
    mine,
    lengths,
    acts,
    weighted,
    loaded,
    order,
    *refs,
):
    del order
    if mine:
        out, block_of, acts_buf, acc, acts_sem = refs
    else:
        out, ahead, block_of, acts_buf, acc, acts_sem, ahead_sem = refs
    rep = lax.axis_index("rep")
    core = lax.rem(rep, 2)
    first_column = lax.div(rep, 2) * 2 * width
    my_column = pl.multiple_of(first_column + core * width, width)
    column = my_column if mine else pl.multiple_of(first_column + (1 - core) * width, width)
    steps = live_blocks(lengths, block_of, span)
    trips = lax.div(steps, 4)
    rest = lax.rem(steps, 4)
    step_rows = STEP_BLOCKS * TOKEN_BLOCK
    trip_rows = 4 * step_rows
    slots = acts_buf.shape[0]
    held = trips + jnp.where(rest > 0, 1, 0)

    def start(trip):
        slot = lax.rem(trip, slots)
        start_acts(
            acts, acts_buf.at[slot], acts_sem.at[slot], block_of, 4 * trip, column, 4 * STEP_BLOCKS
        )

    @pl.when((trips < 2) & (held > 1))
    def _():
        start(jnp.int32(1))

    for early in range(2, slots + 1):
        @pl.when(early < held)
        def _():
            start(jnp.int32(early))

    acc[...] = product(weighted[:, :trip_rows], loaded[0])
    if not mine:
        start_ahead(acts, ahead, ahead_sem, block_of, steps, my_column)

    @pl.when(trips > 1)
    def _():
        acc[...] += product(weighted[:, trip_rows : 2 * trip_rows], loaded[1])

    def body(trip, carry):
        @pl.when(trip + slots - 1 < held)
        def _():
            start(trip + slots - 1)

        slot = lax.rem(trip, slots)
        wait_acts(acts, acts_buf.at[slot], acts_sem.at[slot])
        lanes = pl.ds(pl.multiple_of(trip * trip_rows, trip_rows), trip_rows)
        acc[...] += product(weighted[:, lanes], acts_buf[slot])
        return carry

    lax.fori_loop(2, trips, body, 0)
    slot = lax.rem(trips, slots)
    begin = trips * trip_rows

    @pl.when(rest > 0)
    def _():
        wait_acts(acts, acts_buf.at[slot], acts_sem.at[slot])

    @pl.when(rest > 1)
    def _():
        lanes = pl.ds(pl.multiple_of(begin, trip_rows), 2 * step_rows)
        acc[...] += product(weighted[:, lanes], acts_buf[slot, : 2 * step_rows])

    @pl.when(lax.rem(rest, 2) == 1)
    def _():
        skipped = pl.multiple_of((rest - 1) * step_rows, 2 * step_rows)
        lanes = pl.ds(pl.multiple_of(begin + skipped, 2 * step_rows), step_rows)
        acc[...] += product(weighted[:, lanes], acts_buf[slot, pl.ds(skipped, step_rows)])

    out[...] = acc[...].astype(out.dtype)
    if not mine:
        wait_ahead(acts, ahead, ahead_sem, steps)


def update_kernel(
    own, from_core, from_chip, master, first, second, kept, sent,
    new_master, new_first, new_second, partial_kept, partial_sent,
):
    for tile in range(own.shape[0] // QUANT):
        part = slice(tile * QUANT, (tile + 1) * QUANT)
        total = own[part] + from_core[part].astype(jnp.float32) + from_chip[part].astype(jnp.float32)
        gradient = total.T
        moved_first = beta_one * first[:, part] + (1.0 - beta_one) * gradient
        moved_second = beta_two * second[:, part] + (1.0 - beta_two) * gradient * gradient
        corrected_first = moved_first * (learn_rate / (1.0 - beta_one**steps_done))
        corrected_second = moved_second * (1.0 / (1.0 - beta_two**steps_done))
        moved = master[:, part] * (1.0 - learn_rate * weight_decay) - corrected_first / (
            jnp.sqrt(corrected_second) + epsilon
        )
        new_first[:, part] = moved_first
        new_second[:, part] = moved_second
        new_master[:, part] = moved
        largest = jnp.max(jnp.abs(moved), axis=1, keepdims=True)
        scales = ((largest + scale_epsilon) / quant_top).astype(jnp.bfloat16).astype(jnp.float32)
        quantized = (moved * (1.0 / scales)).astype(jnp.bfloat16).astype(jnp.float32)
        used = quantized * scales
        high = used.astype(jnp.bfloat16)
        low = (used - high.astype(jnp.float32)).astype(jnp.bfloat16)
        partial_sent[:, part] = (product(sent[...], high) + product(sent[...], low)).astype(jnp.bfloat16)
        partial_kept[:, part] = product(kept[...], high) + product(kept[...], low)


def attention_kernel(
    lengths, queries, new_keys, cache_keys, cache_values, master, first, second,
    mixed, late, master_out, first_out, second_out, flat, keys, sems,
):
    writes = [
        pltpu.make_async_copy(source, target, sems.at[place])
        for place, (source, target) in enumerate(
            ((master, master_out), (first, first_out), (second, second_out))
        )
    ]
    for write in writes:
        write.start()
    steps, seqs, _ = queries.shape
    slots = cache_keys.shape[1]
    kv_local = new_keys.shape[2] // HEAD
    group = HEADS // KV_HEADS
    lines = steps * seqs
    for step in range(steps):
        flat[step * seqs : (step + 1) * seqs, :] = queries[step].astype(jnp.float32)
        keys[step * seqs : (step + 1) * seqs, :] = new_keys[step].astype(jnp.float32)
    rows = group * lines

    def index(shape, axis):
        return lax.broadcasted_iota(jnp.int32, shape, axis)

    wide_shape = (rows, slots)
    seq_of = lax.rem(index(wide_shape, 0), seqs)
    limit = jnp.zeros(wide_shape, jnp.int32)
    for seq in range(seqs):
        limit = jnp.where(seq_of == seq, lengths[seq], limit)
    live = index(wide_shape, 1) < limit
    late_shape = (rows, lines)
    late_row = index(late_shape, 0)
    late_col = index(late_shape, 1)
    allowed = (lax.rem(late_row, seqs) == lax.rem(late_col, seqs)) & (
        lax.div(late_col, seqs) <= lax.rem(lax.div(late_row, seqs), steps)
    )
    score_scale = HEAD ** (-0.5)
    across = (((1,), (1,)), ((), ()))
    for head in range(kv_local):
        lanes = slice(head * HEAD, (head + 1) * HEAD)
        query = jnp.concatenate(
            [
                flat[:, (head * group + part) * HEAD : (head * group + part + 1) * HEAD]
                for part in range(group)
            ],
            axis=0,
        ).astype(jnp.bfloat16)
        scores = jnp.zeros(wide_shape, jnp.float32)
        for seq in range(seqs):
            one = lax.dot_general(
                query, cache_keys[seq, :, lanes], across, preferred_element_type=jnp.float32
            )
            scores = jnp.where(seq_of == seq, one, scores)
        scores = jnp.where(live, scores * score_scale, -jnp.inf)
        scores_new = (
            lax.dot_general(
                query, keys[:, lanes].astype(jnp.bfloat16), across, preferred_element_type=jnp.float32
            )
            * score_scale
        )
        scores_new = jnp.where(allowed, scores_new, -jnp.inf)
        highest = jnp.maximum(
            jnp.max(scores, axis=1, keepdims=True), jnp.max(scores_new, axis=1, keepdims=True)
        )
        exp_cache = jnp.exp(scores - highest)
        exp_new = jnp.exp(scores_new - highest)
        totals = jnp.sum(exp_cache, axis=1, keepdims=True) + jnp.sum(exp_new, axis=1, keepdims=True)
        probs = exp_cache / totals
        late[head] = (exp_new / totals).astype(jnp.bfloat16)
        result = jnp.zeros((rows, HEAD), jnp.float32)
        for seq in range(seqs):
            mine = jnp.where(seq_of == seq, probs, 0.0).astype(jnp.bfloat16)
            result = result + jnp.dot(
                mine, cache_values[seq, :, lanes], preferred_element_type=jnp.float32
            )
        mixed[head] = result
    for write in writes:
        write.wait()


def finish_kernel(steps, seqs, *refs):
    mixed, late, own = refs[:3]
    arrived = refs[3:-3]
    new_values, attended, flat = refs[-3:]
    total = own[...]
    for block in arrived:
        total = total + block[...].astype(jnp.float32)
    values = total.astype(jnp.bfloat16)
    wide_values = values.astype(jnp.float32)
    lines = steps * seqs
    kv_local, rows, _ = mixed.shape
    group = rows // lines
    for head in range(kv_local):
        lanes = slice(head * HEAD, (head + 1) * HEAD)
        result = mixed[head] + jnp.dot(late[head], values[:, lanes], preferred_element_type=jnp.float32)
        for part in range(group):
            flat[:, (head * group + part) * HEAD : (head * group + part + 1) * HEAD] = result[
                part * lines : (part + 1) * lines, :
            ]
    for step in range(steps):
        new_values[step] = wide_values[step * seqs : (step + 1) * seqs, :].astype(jnp.bfloat16)
        attended[step] = flat[step * seqs : (step + 1) * seqs, :].astype(jnp.bfloat16)


HBM = pl.BlockSpec(memory_space=pltpu.HBM)
VMEM = pl.BlockSpec(memory_space=pltpu.VMEM)
SMEM = pl.BlockSpec(memory_space=pltpu.SMEM)
PARAMS = pltpu.CompilerParams(vmem_limit_bytes=24 * 1024 * 1024)


def on_device(
    activations,
    value_grads,
    seq_lengths,
    master,
    first_moment,
    second_moment,
    hidden,
    queries,
    new_keys,
    cache_keys,
    cache_values,
    cache_lengths,
):
    shape = jax.ShapeDtypeStruct
    bf16, f32 = jnp.bfloat16, jnp.float32
    wide_count = lax.axis_size("wide")
    rep_count = lax.axis_size("rep")
    tokens, cols = value_grads.shape
    seqs = seq_lengths.shape[0]
    span = tokens // seqs
    step_count, row_local, _ = hidden.shape
    lines = step_count * row_local
    width = master.shape[0]
    blocks = tokens // TOKEN_BLOCK + PAD
    step_rows = STEP_BLOCKS * TOKEN_BLOCK

    core_pairs = [(i, i ^ 1) for i in range(rep_count)]
    chip_pairs = [(i, i ^ 2) for i in range(rep_count)]

    table = pltpu.SMEM((blocks,), jnp.int32)

    def buffers(rows, columns):
        return pltpu.VMEM((BUFFERS, rows, columns), bf16)

    sems = pltpu.SemaphoreType.DMA((BUFFERS,))
    ours, for_core, weighted, pieces, ahead = pl.pallas_call(
        functools.partial(first_kernel, span, width, wide_count, rep_count),
        out_shape=(
            shape((cols, width), f32),
            shape((cols, width), bf16),
            pltpu.VMEM((cols, tokens + step_rows), bf16),
            shape((4, wide_count, lines, width), bf16),
            pltpu.VMEM((2, 4 * step_rows, width), bf16),
        ),
        in_specs=[HBM, HBM, HBM, HBM],
        out_specs=(VMEM,) * 5,
        scratch_shapes=[
            pltpu.SMEM(seq_lengths.shape, jnp.int32),
            table,
            table,
            table,
            buffers(step_rows, 2 * width),
            buffers(step_rows, cols),
            pltpu.VMEM((cols, step_rows), bf16),
            pltpu.VMEM((cols, step_rows), bf16),
            pltpu.VMEM((cols, 2 * width), f32),
            pltpu.VMEM(hidden.shape, bf16),
            pltpu.VMEM((lines, hidden.shape[2]), f32),
            sems,
            sems,
            pltpu.SemaphoreType.DMA,
            pltpu.SemaphoreType.DMA,
            pltpu.SemaphoreType.DMA((2,)),
        ],
        compiler_params=PARAMS,
        name="first_chunk",
    )(in_hbm(seq_lengths), activations, in_hbm(value_grads), in_hbm(hidden))
    core_part = lax.ppermute(for_core, "rep", core_pairs)
    both_pairs = [(i, i ^ 3) for i in range(rep_count)]
    moved = jnp.stack(
        [
            pieces[0],
            lax.ppermute(pieces[1], "rep", chip_pairs),
            lax.ppermute(pieces[2], "rep", core_pairs),
            lax.ppermute(pieces[3], "rep", both_pairs),
        ]
    )

    for_chip = (ours + core_part.astype(f32)).astype(bf16)
    chip_part = lax.ppermute(for_chip, "rep", chip_pairs)

    def own_call(mine, ahead, order, out_shape):
        return pl.pallas_call(
            functools.partial(own_kernel, span, width, mine),
            out_shape=out_shape,
            in_specs=[SMEM, HBM, VMEM, VMEM, HBM],
            out_specs=(VMEM,) * len(out_shape),
            scratch_shapes=[
                table,
                pltpu.VMEM((3, 4 * step_rows, width), bf16),
                pltpu.VMEM((cols, width), f32),
                pltpu.SemaphoreType.DMA((3,)),
            ]
            + [pltpu.SemaphoreType.DMA((2,))] * (not mine),
            compiler_params=PARAMS,
            name="own_chunk" if mine else "near_chunk",
        )(seq_lengths, activations, weighted, ahead, order)

    for_core, ahead = own_call(
        False, ahead, for_chip, (shape((cols, width), bf16), pltpu.VMEM((2, 4 * step_rows, width), bf16))
    )
    core_part = lax.ppermute(for_core, "rep", core_pairs)
    pieces = [moved[:, 0]]
    for dz in range(1, wide_count):
        pairs = [(i, i ^ dz) for i in range(wide_count)]
        pieces.append(lax.ppermute(moved[:, dz], "wide", pairs))
    moved = jnp.stack(pieces, axis=1)
    group_rows = 2 * wide_count * lines
    hidden_kept = moved[:2].reshape(group_rows, width)
    hidden_sent = moved[2:].reshape(group_rows, width)

    (own_part,) = own_call(True, ahead, for_core, (shape((cols, width), f32),))
    new_master, new_first, new_second, kept, sent = pl.pallas_call(
        update_kernel,
        out_shape=(pltpu.VMEM((width, cols), f32),) * 3
        + (shape((group_rows, cols), f32), shape((group_rows, cols), bf16)),
        in_specs=[VMEM] * 8,
        out_specs=(VMEM,) * 5,
        compiler_params=PARAMS,
        name="update",
    )(own_part, core_part, chip_part, master, first_moment, second_moment, hidden_kept, hidden_sent)
    summed = kept + lax.ppermute(sent, "rep", core_pairs).astype(f32)
    half = wide_count * lines
    summed = summed[:half] + lax.ppermute(summed[half:].astype(bf16), "rep", chip_pairs).astype(f32)
    arrived = []
    for place in range(1, wide_count):
        pairs = [(i, i ^ place) for i in range(wide_count)]
        arrived.append(
            lax.ppermute(summed[place * lines : (place + 1) * lines].astype(bf16), "wide", pairs)
        )
    kv_local = cols // HEAD
    rows = (HEADS // KV_HEADS) * lines
    mixed, late, new_master, new_first, new_second = pl.pallas_call(
        attention_kernel,
        out_shape=(
            shape((kv_local, rows, HEAD), f32),
            shape((kv_local, rows, lines), bf16),
            *(pltpu.HBM((width, cols), f32),) * 3,
        ),
        in_specs=[SMEM] + [VMEM] * 7,
        out_specs=(VMEM, VMEM, HBM, HBM, HBM),
        scratch_shapes=[
            pltpu.VMEM((lines, queries.shape[2]), f32),
            pltpu.VMEM((lines, cols), f32),
            pltpu.SemaphoreType.DMA((3,)),
        ],
        compiler_params=PARAMS,
        name="cache_attention",
    )(cache_lengths, queries, new_keys, cache_keys, cache_values, new_master, new_first, new_second)
    new_values, attended = pl.pallas_call(
        functools.partial(finish_kernel, step_count, row_local),
        out_shape=(shape(new_keys.shape, bf16), shape(queries.shape, bf16)),
        in_specs=[VMEM] * (3 + len(arrived)),
        out_specs=(VMEM, VMEM),
        scratch_shapes=[pltpu.VMEM((lines, queries.shape[2]), f32)],
        compiler_params=PARAMS,
        name="finish",
    )(mixed, late, summed[:lines], *arrived)
    return (new_master, new_first, new_second, new_values, attended)


def in_hbm(value):
    return pltpu.with_memory_space_constraint(value, pltpu.HBM)


def dispatch(*args):
    _, value_grads, seq_lengths, master, _, _, hidden = args[:7]
    lines = hidden.shape[0] * hidden.shape[1]
    wide_count = lax.axis_size("wide")
    fits = (
        lax.axis_size("rep") == 4
        and wide_count & (wide_count - 1) == 0
        and master.shape[0] % 128 == 0
        and master.shape[1] % QUANT == 0
        and (value_grads.shape[0] // seq_lengths.shape[0]) % TOKEN_BLOCK == 0
        and lines == 16
        and seq_lengths.shape[0] >= STEP_BLOCKS
        and seq_lengths.shape[0] % STEP_BLOCKS == 0
        and seq_lengths.shape[0] < BUFFERS * STEP_BLOCKS
    )
    if not fits:
        return on_device_plain(*args)
    return on_device(*args)


def solution(mesh):
    in_specs = (
        P("rep", "wide"),
        P("rep", "tp"),
        P("rep"),
        P(("wide", "rep"), "tp"),
        P(("wide", "rep"), "tp"),
        P(("wide", "rep"), "tp"),
        P(None, ("wide", "rep"), None),
        P(None, ("wide", "rep"), "tp"),
        P(None, ("wide", "rep"), "tp"),
        P(("wide", "rep"), None, "tp"),
        P(("wide", "rep"), None, "tp"),
        P(("wide", "rep")),
    )
    out_specs = (
        P(("wide", "rep"), "tp"),
        P(("wide", "rep"), "tp"),
        P(("wide", "rep"), "tp"),
        P(None, ("wide", "rep"), "tp"),
        P(None, ("wide", "rep"), "tp"),
    )
    return jax.shard_map(
        dispatch, mesh=mesh, in_specs=in_specs, out_specs=out_specs, check_vma=False
    )
```

```python
import functools

import jax
import jax.numpy as jnp
from jax import lax
from jax.experimental import pallas as pl
from jax.experimental.pallas import tpu as pltpu
from jax.sharding import PartitionSpec as P


HEADS = 64
KV_HEADS = 8
HEAD = 128
QUANT = 128


beta_one = 0.9
beta_two = 0.95
learn_rate = 0.001
weight_decay = 0.1
epsilon = 1e-08
steps_done = 10.0
quant_top = 448.0
scale_epsilon = 1e-06


def quantize(weights):
    row_count, col_count = weights.shape
    tiled = weights.reshape(row_count, col_count // QUANT, QUANT)
    largest = jnp.max(jnp.abs(tiled), axis=2)
    scales = ((largest + scale_epsilon) / quant_top).astype(jnp.bfloat16)
    quantized = (tiled / scales.astype(jnp.float32)[:, :, None]).astype(jnp.bfloat16)
    return (quantized.reshape(row_count, col_count), scales)


def dequantize(quantized, scales):
    row_count, col_count = quantized.shape
    tiled = quantized.astype(jnp.float32).reshape(row_count, col_count // QUANT, QUANT)
    return (tiled * scales.astype(jnp.float32)[:, :, None]).reshape(row_count, col_count)


def on_device_plain(
    activations,
    value_grads,
    seq_lengths,
    master,
    first_moment,
    second_moment,
    hidden,
    queries,
    new_keys,
    cache_keys,
    cache_values,
    cache_lengths,
):
    seq_count = seq_lengths.shape[0]
    token_count, col_count = value_grads.shape
    seq_span = token_count // seq_count
    position = jnp.arange(seq_span, dtype=jnp.int32)
    lengths = seq_lengths.astype(jnp.float32)
    token_weight = jnp.where(position[None, :] < seq_lengths[:, None], 1.0 / lengths[:, None], 0.0)
    weighted = (
        value_grads.astype(jnp.float32).reshape(seq_count, seq_span, col_count)
        * token_weight[:, :, None]
    ).astype(jnp.bfloat16)
    weighted = weighted.reshape(token_count, col_count)
    gradient = lax.psum_scatter(
        lax.dot_general(
            activations, weighted, (((0,), (0,)), ((), ())), preferred_element_type=jnp.float32
        ),
        "rep",
        scatter_dimension=0,
        tiled=True,
    )
    new_first = beta_one * first_moment + (1.0 - beta_one) * gradient
    new_second = beta_two * second_moment + (1.0 - beta_two) * gradient * gradient
    corrected_first = new_first / (1.0 - beta_one**steps_done)
    corrected_second = new_second / (1.0 - beta_two**steps_done)
    new_master = master - learn_rate * (
        corrected_first / (jnp.sqrt(corrected_second) + epsilon) + weight_decay * master
    )
    quantized, scales = quantize(new_master)
    step_count, row_local, width = hidden.shape
    score_scale = HEAD ** (-0.5)
    group = HEADS // KV_HEADS
    kv_local = col_count // HEAD
    query = queries.reshape(step_count, row_local, kv_local, group, HEAD)
    keys_cache = cache_keys.reshape(row_local, cache_keys.shape[1], kv_local, HEAD)
    values_cache = cache_values.reshape(row_local, cache_values.shape[1], kv_local, HEAD)
    keys_new = new_keys.reshape(step_count, row_local, kv_local, HEAD)
    slots = jnp.arange(cache_keys.shape[1], dtype=jnp.int32)
    cache_live = slots[None, :] < cache_lengths[:, None]
    scores_cache = (
        jnp.einsum("sbgrd,bjgd->sbgrj", query, keys_cache, preferred_element_type=jnp.float32)
        * score_scale
    )
    scores_cache = jnp.where(cache_live[None, :, None, None, :], scores_cache, -jnp.inf)
    scores_new = (
        jnp.einsum("sbgrd,tbgd->sbgrt", query, keys_new, preferred_element_type=jnp.float32)
        * score_scale
    )
    moments = jnp.arange(step_count, dtype=jnp.int32)
    earlier = moments[None, :] <= moments[:, None]
    scores_new = jnp.where(earlier[:, None, None, None, :], scores_new, -jnp.inf)
    highest = jnp.maximum(jnp.max(scores_cache, axis=4), jnp.max(scores_new, axis=4))
    exp_cache = jnp.exp(scores_cache - highest[..., None])
    exp_new = jnp.exp(scores_new - highest[..., None])
    totals = jnp.sum(exp_cache, axis=4) + jnp.sum(exp_new, axis=4)
    probs_cache = (exp_cache / totals[..., None]).astype(jnp.bfloat16)
    probs_new = (exp_new / totals[..., None]).astype(jnp.bfloat16)
    mixed_cache = jnp.einsum(
        "sbgrj,bjgd->sbgrd", probs_cache, values_cache, preferred_element_type=jnp.float32
    )
    wide_count = lax.axis_size("wide")
    rep_count = lax.axis_size("rep")
    block_rows = width // (wide_count * rep_count)
    arranged = hidden.reshape(step_count, row_local, wide_count, rep_count, block_rows)
    swapped = lax.all_to_all(arranged, "rep", split_axis=3, concat_axis=1, tiled=True)
    group_rows = rep_count * row_local
    flat_group = swapped.reshape(step_count * group_rows, wide_count * block_rows).astype(
        jnp.float32
    )
    quant_rows = lax.all_gather(quantized, "wide", axis=0, tiled=True)
    scale_rows = lax.all_gather(scales, "wide", axis=0, tiled=True)
    weight_rows = dequantize(quant_rows, scale_rows)
    partial_value = jnp.dot(
        flat_group, weight_rows, precision=lax.Precision.HIGHEST, preferred_element_type=jnp.float32
    )
    partial_value = partial_value.reshape(step_count, group_rows, col_count)
    projected = lax.psum_scatter(partial_value, "rep", scatter_dimension=1, tiled=True)
    new_values = projected.astype(jnp.bfloat16)
    values_new = new_values.reshape(step_count, row_local, kv_local, HEAD)
    mixed = mixed_cache + jnp.einsum(
        "sbgrt,tbgd->sbgrd", probs_new, values_new, preferred_element_type=jnp.float32
    )
    attended = mixed.astype(jnp.bfloat16).reshape(step_count, row_local, kv_local * group * HEAD)
    return (new_master, new_first, new_second, new_values, attended)


TOKEN_BLOCK = 128
STEP_BLOCKS = 4
BUFFERS = 7
TRIP_STEPS = 4
PAD = TRIP_STEPS * STEP_BLOCKS


def live_blocks(lengths, block_of, span):
    per_seq = span // TOKEN_BLOCK
    seqs = lengths.shape[0]
    for seq in range(seqs):
        block_of[seq] = seq * per_seq
    count = jnp.int32(seqs)
    for seq in range(seqs):
        length = lengths[seq]
        for part in range(1, per_seq):
            block_of[count] = seq * per_seq + part
            count = count + jnp.where(length > part * TOKEN_BLOCK, 1, 0)
    for pad in range(PAD):
        block_of[count + pad] = 0
    return count, jnp.maximum(lax.div(count + STEP_BLOCKS - 1, STEP_BLOCKS), TRIP_STEPS)


def start_acts(acts, buf, sem, block_of, step, column, parts):
    width = buf.shape[1]
    for part in range(parts):
        first = pl.multiple_of(block_of[step * STEP_BLOCKS + part] * TOKEN_BLOCK, TOKEN_BLOCK)
        pltpu.make_async_copy(
            acts.at[pl.ds(first, TOKEN_BLOCK), pl.ds(column, width)],
            buf.at[part * TOKEN_BLOCK : (part + 1) * TOKEN_BLOCK],
            sem,
        ).start()


def wait_acts(acts, buf, sem):
    rows, cols = buf.shape
    pltpu.make_async_copy(acts.at[pl.ds(0, rows), pl.ds(0, cols)], buf, sem).wait()


def start_ahead(acts, ahead, sem, block_of, steps, column):
    start_acts(acts, ahead.at[0], sem.at[0], block_of, 0, column, TRIP_STEPS * STEP_BLOCKS)

    @pl.when(steps >= 2 * TRIP_STEPS)
    def _():
        start_acts(
            acts, ahead.at[1], sem.at[1], block_of, TRIP_STEPS, column, TRIP_STEPS * STEP_BLOCKS
        )


def wait_ahead(acts, ahead, sem, steps):
    wait_acts(acts, ahead.at[0], sem.at[0])

    @pl.when(steps >= 2 * TRIP_STEPS)
    def _():
        wait_acts(acts, ahead.at[1], sem.at[1])


def product(left, right):
    return jnp.dot(left, right, preferred_element_type=jnp.float32)


def first_kernel(
    span,
    width,
    wide_count,
    rep_count,
    lengths_in,
    acts,
    grads,
    hidden,
    ours,
    theirs,
    weighted,
    pieces,
    ahead,
    lengths,
    block_of,
    acts_buf,
    grads_buf,
    even,
    odd,
    acc,
    loaded,
    flat,
    acts_sem,
    grads_sem,
    hidden_sem,
    lengths_sem,
    ahead_sem,
):
    rep = lax.axis_index("rep")
    here = lax.axis_index("wide")
    core = lax.rem(rep, 2)
    chip = lax.div(rep, 2)
    column = pl.multiple_of((1 - chip) * 2 * width, 2 * width)
    next_column = pl.multiple_of((chip * 2 + 1 - core) * width, width)
    step_rows = STEP_BLOCKS * TOKEN_BLOCK
    cols = grads.shape[1]
    fetch_lengths = pltpu.make_async_copy(lengths_in, lengths, lengths_sem)
    fetch_lengths.start()

    def start(step, blocks=block_of):
        slot = step % BUFFERS if isinstance(step, int) else lax.rem(step, BUFFERS)
        start_acts(grads, grads_buf.at[slot], grads_sem.at[slot], blocks, step, 0, STEP_BLOCKS)
        start_acts(acts, acts_buf.at[slot], acts_sem.at[slot], blocks, step, column, STEP_BLOCKS)

    per_seq = span // TOKEN_BLOCK
    per_seq_bits = per_seq.bit_length() - 1
    known = [seq * per_seq for seq in range(lengths.shape[0])]
    known_steps = len(known) // STEP_BLOCKS
    start(0, known)
    fetch = pltpu.make_async_copy(hidden, loaded, hidden_sem)
    fetch.start()
    for early in range(1, known_steps):
        start(early, known)

    def turn(step, target):
        slot = lax.rem(step, BUFFERS)
        for part in range(STEP_BLOCKS):
            entry = step * STEP_BLOCKS + part
            rows = slice(part * TOKEN_BLOCK, (part + 1) * TOKEN_BLOCK)
            value = grads_buf[slot, rows, :].astype(jnp.float32)
            block = block_of[entry]
            seq_length = lengths[block >> per_seq_bits]
            limit = jnp.where(entry < count, seq_length - (block & (per_seq - 1)) * TOKEN_BLOCK, 0)
            length = jnp.full((1, cols), seq_length, jnp.int32).astype(jnp.float32)
            position = lax.broadcasted_iota(jnp.int32, value.shape, 0)
            scaled = jnp.where(position < limit, value * (1.0 / length), 0.0)
            turned = scaled.astype(jnp.bfloat16).T
            target[:, rows] = turned
            place = pl.multiple_of(step * step_rows + part * TOKEN_BLOCK, TOKEN_BLOCK)
            weighted[:, pl.ds(place, TOKEN_BLOCK)] = turned

    acc[...] = jnp.zeros_like(acc)
    fetch_lengths.wait()
    count, steps = live_blocks(lengths, block_of, span)
    for early in range(known_steps, BUFFERS - 1):
        @pl.when(early < steps)
        def _():
            start(early)

    fetch.wait()
    groups, rows, _ = loaded.shape
    for step in range(groups):
        flat[step * rows : (step + 1) * rows, :] = loaded[step].astype(jnp.float32)
    for dc in range(2):
        for dx in range(2):
            for dz in range(wide_count):
                place = (here ^ dz) * rep_count + (chip ^ dx) * 2 + (core ^ dc)
                begin = pl.multiple_of(place * width, width)
                pieces[dc * 2 + dx, dz] = flat[:, pl.ds(begin, width)].astype(jnp.bfloat16)

    wait_acts(grads, grads_buf.at[0], grads_sem.at[0])
    turn(jnp.int32(0), even)

    def phase(step, source, target):
        @pl.when(step + BUFFERS - 1 < steps)
        def _():
            start(step + BUFFERS - 1)

        @pl.when(step + 1 < steps)
        def _():
            slot = lax.rem(step + 1, BUFFERS)
            wait_acts(grads, grads_buf.at[slot], grads_sem.at[slot])

        slot = lax.rem(step, BUFFERS)
        wait_acts(acts, acts_buf.at[slot], acts_sem.at[slot])
        turn(step + 1, target)
        acc[...] += product(source[...], acts_buf[slot])

    def body(pair, carry):
        for trip in range(2):
            @pl.when((pair == 2 * trip + 1) & (steps >= (trip + 1) * TRIP_STEPS))
            def _():
                start_acts(
                    acts,
                    ahead.at[trip],
                    ahead_sem.at[trip],
                    block_of,
                    trip * TRIP_STEPS,
                    next_column,
                    TRIP_STEPS * STEP_BLOCKS,
                )

        phase(2 * pair, even, odd)
        phase(2 * pair + 1, odd, even)
        return carry

    lax.fori_loop(0, lax.div(steps, 2), body, 0)

    @pl.when(lax.rem(steps, 2) == 1)
    def _():
        slot = lax.rem(steps - 1, BUFFERS)
        wait_acts(acts, acts_buf.at[slot], acts_sem.at[slot])
        acc[...] += product(even[...], acts_buf[slot])

    split(acc, core, ours, theirs)
    wait_ahead(acts, ahead, ahead_sem, steps)


def split(acc, core, ours, theirs):
    width = ours.shape[1]
    ours[...] = acc[:, pl.ds(pl.multiple_of(core * width, width), width)]
    theirs[...] = acc[:, pl.ds(pl.multiple_of((1 - core) * width, width), width)].astype(jnp.bfloat16)


def own_kernel(
    span,
    width,
    mine,
    lengths,
    acts,
    weighted,
    loaded,
    order,
    *refs,
):
    del order
    if mine:
        out, block_of, acts_buf, acc, acts_sem = refs
    else:
        out, ahead, block_of, acts_buf, acc, acts_sem, ahead_sem = refs
    rep = lax.axis_index("rep")
    core = lax.rem(rep, 2)
    first_column = lax.div(rep, 2) * 2 * width
    my_column = pl.multiple_of(first_column + core * width, width)
    column = my_column if mine else pl.multiple_of(first_column + (1 - core) * width, width)
    _, steps = live_blocks(lengths, block_of, span)
    trips = lax.div(steps, 4)
    rest = lax.rem(steps, 4)
    step_rows = STEP_BLOCKS * TOKEN_BLOCK
    trip_rows = 4 * step_rows
    slots = acts_buf.shape[0]
    held = trips + jnp.where(rest > 0, 1, 0)

    def start(trip):
        slot = lax.rem(trip, slots)
        start_acts(
            acts, acts_buf.at[slot], acts_sem.at[slot], block_of, 4 * trip, column, 4 * STEP_BLOCKS
        )

    @pl.when((trips < 2) & (held > 1))
    def _():
        start(jnp.int32(1))

    for early in range(2, slots + 1):
        @pl.when(early < held)
        def _():
            start(jnp.int32(early))

    acc[...] = product(weighted[:, :trip_rows], loaded[0])
    if not mine:
        start_ahead(acts, ahead, ahead_sem, block_of, steps, my_column)

    @pl.when(trips > 1)
    def _():
        acc[...] += product(weighted[:, trip_rows : 2 * trip_rows], loaded[1])

    def body(trip, carry):
        @pl.when(trip + slots - 1 < held)
        def _():
            start(trip + slots - 1)

        slot = lax.rem(trip, slots)
        wait_acts(acts, acts_buf.at[slot], acts_sem.at[slot])
        lanes = pl.ds(pl.multiple_of(trip * trip_rows, trip_rows), trip_rows)
        acc[...] += product(weighted[:, lanes], acts_buf[slot])
        return carry

    lax.fori_loop(2, trips, body, 0)
    slot = lax.rem(trips, slots)
    begin = trips * trip_rows

    @pl.when(rest > 0)
    def _():
        wait_acts(acts, acts_buf.at[slot], acts_sem.at[slot])

    @pl.when(rest > 1)
    def _():
        lanes = pl.ds(pl.multiple_of(begin, trip_rows), 2 * step_rows)
        acc[...] += product(weighted[:, lanes], acts_buf[slot, : 2 * step_rows])

    @pl.when(lax.rem(rest, 2) == 1)
    def _():
        skipped = pl.multiple_of((rest - 1) * step_rows, 2 * step_rows)
        lanes = pl.ds(pl.multiple_of(begin + skipped, 2 * step_rows), step_rows)
        acc[...] += product(weighted[:, lanes], acts_buf[slot, pl.ds(skipped, step_rows)])

    out[...] = acc[...].astype(out.dtype)
    if not mine:
        wait_ahead(acts, ahead, ahead_sem, steps)


def update_kernel(
    own, from_core, from_chip, master, first, second, kept, sent,
    new_master, new_first, new_second, partial_kept, partial_sent,
):
    for tile in range(own.shape[0] // QUANT):
        part = slice(tile * QUANT, (tile + 1) * QUANT)
        total = own[part] + from_core[part].astype(jnp.float32) + from_chip[part].astype(jnp.float32)
        gradient = total.T
        moved_first = beta_one * first[:, part] + (1.0 - beta_one) * gradient
        moved_second = beta_two * second[:, part] + (1.0 - beta_two) * gradient * gradient
        corrected_first = moved_first * (learn_rate / (1.0 - beta_one**steps_done))
        corrected_second = moved_second * (1.0 / (1.0 - beta_two**steps_done))
        moved = master[:, part] * (1.0 - learn_rate * weight_decay) - corrected_first / (
            jnp.sqrt(corrected_second) + epsilon
        )
        new_first[:, part] = moved_first
        new_second[:, part] = moved_second
        new_master[:, part] = moved
        largest = jnp.max(jnp.abs(moved), axis=1, keepdims=True)
        scales = ((largest + scale_epsilon) / quant_top).astype(jnp.bfloat16).astype(jnp.float32)
        quantized = (moved * (1.0 / scales)).astype(jnp.bfloat16).astype(jnp.float32)
        used = quantized * scales
        high = used.astype(jnp.bfloat16)
        low = (used - high.astype(jnp.float32)).astype(jnp.bfloat16)
        partial_sent[:, part] = (product(sent[...], high) + product(sent[...], low)).astype(jnp.bfloat16)
        partial_kept[:, part] = product(kept[...], high) + product(kept[...], low)


def attention_kernel(
    lengths, queries, new_keys, cache_keys, cache_values, master, first, second,
    mixed, late, master_out, first_out, second_out, flat, keys, sems,
):
    writes = [
        pltpu.make_async_copy(source, target, sems.at[place])
        for place, (source, target) in enumerate(
            ((master, master_out), (first, first_out), (second, second_out))
        )
    ]
    for write in writes:
        write.start()
    steps, seqs, _ = queries.shape
    slots = cache_keys.shape[1]
    kv_local = new_keys.shape[2] // HEAD
    group = HEADS // KV_HEADS
    lines = steps * seqs
    for step in range(steps):
        flat[step * seqs : (step + 1) * seqs, :] = queries[step].astype(jnp.float32)
        keys[step * seqs : (step + 1) * seqs, :] = new_keys[step].astype(jnp.float32)
    rows = group * lines

    def index(shape, axis):
        return lax.broadcasted_iota(jnp.int32, shape, axis)

    wide_shape = (rows, slots)
    seq_of = lax.rem(index(wide_shape, 0), seqs)
    limit = jnp.zeros(wide_shape, jnp.int32)
    for seq in range(seqs):
        limit = jnp.where(seq_of == seq, lengths[seq], limit)
    live = index(wide_shape, 1) < limit
    late_shape = (rows, lines)
    late_row = index(late_shape, 0)
    late_col = index(late_shape, 1)
    allowed = (lax.rem(late_row, seqs) == lax.rem(late_col, seqs)) & (
        lax.div(late_col, seqs) <= lax.rem(lax.div(late_row, seqs), steps)
    )
    score_scale = HEAD ** (-0.5)
    across = (((1,), (1,)), ((), ()))
    for head in range(kv_local):
        lanes = slice(head * HEAD, (head + 1) * HEAD)
        query = jnp.concatenate(
            [
                flat[:, (head * group + part) * HEAD : (head * group + part + 1) * HEAD]
                for part in range(group)
            ],
            axis=0,
        ).astype(jnp.bfloat16)
        scores = jnp.zeros(wide_shape, jnp.float32)
        for seq in range(seqs):
            one = lax.dot_general(
                query, cache_keys[seq, :, lanes], across, preferred_element_type=jnp.float32
            )
            scores = jnp.where(seq_of == seq, one, scores)
        scores = jnp.where(live, scores * score_scale, -jnp.inf)
        scores_new = (
            lax.dot_general(
                query, keys[:, lanes].astype(jnp.bfloat16), across, preferred_element_type=jnp.float32
            )
            * score_scale
        )
        scores_new = jnp.where(allowed, scores_new, -jnp.inf)
        highest = jnp.maximum(
            jnp.max(scores, axis=1, keepdims=True), jnp.max(scores_new, axis=1, keepdims=True)
        )
        exp_cache = jnp.exp(scores - highest)
        exp_new = jnp.exp(scores_new - highest)
        totals = jnp.sum(exp_cache, axis=1, keepdims=True) + jnp.sum(exp_new, axis=1, keepdims=True)
        probs = exp_cache / totals
        late[head] = (exp_new / totals).astype(jnp.bfloat16)
        result = jnp.zeros((rows, HEAD), jnp.float32)
        for seq in range(seqs):
            mine = jnp.where(seq_of == seq, probs, 0.0).astype(jnp.bfloat16)
            result = result + jnp.dot(
                mine, cache_values[seq, :, lanes], preferred_element_type=jnp.float32
            )
        mixed[head] = result
    for write in writes:
        write.wait()


def finish_kernel(steps, seqs, *refs):
    mixed, late, own = refs[:3]
    arrived = refs[3:-3]
    new_values, attended, flat = refs[-3:]
    total = own[...]
    for block in arrived:
        total = total + block[...].astype(jnp.float32)
    values = total.astype(jnp.bfloat16)
    wide_values = values.astype(jnp.float32)
    lines = steps * seqs
    kv_local, rows, _ = mixed.shape
    group = rows // lines
    for head in range(kv_local):
        lanes = slice(head * HEAD, (head + 1) * HEAD)
        result = mixed[head] + jnp.dot(late[head], values[:, lanes], preferred_element_type=jnp.float32)
        for part in range(group):
            flat[:, (head * group + part) * HEAD : (head * group + part + 1) * HEAD] = result[
                part * lines : (part + 1) * lines, :
            ]
    for step in range(steps):
        new_values[step] = wide_values[step * seqs : (step + 1) * seqs, :].astype(jnp.bfloat16)
        attended[step] = flat[step * seqs : (step + 1) * seqs, :].astype(jnp.bfloat16)


HBM = pl.BlockSpec(memory_space=pltpu.HBM)
VMEM = pl.BlockSpec(memory_space=pltpu.VMEM)
SMEM = pl.BlockSpec(memory_space=pltpu.SMEM)
PARAMS = pltpu.CompilerParams(vmem_limit_bytes=24 * 1024 * 1024)


def on_device(
    activations,
    value_grads,
    seq_lengths,
    master,
    first_moment,
    second_moment,
    hidden,
    queries,
    new_keys,
    cache_keys,
    cache_values,
    cache_lengths,
):
    shape = jax.ShapeDtypeStruct
    bf16, f32 = jnp.bfloat16, jnp.float32
    wide_count = lax.axis_size("wide")
    rep_count = lax.axis_size("rep")
    tokens, cols = value_grads.shape
    seqs = seq_lengths.shape[0]
    span = tokens // seqs
    step_count, row_local, _ = hidden.shape
    lines = step_count * row_local
    width = master.shape[0]
    blocks = tokens // TOKEN_BLOCK + PAD
    step_rows = STEP_BLOCKS * TOKEN_BLOCK

    core_pairs = [(i, i ^ 1) for i in range(rep_count)]
    chip_pairs = [(i, i ^ 2) for i in range(rep_count)]

    table = pltpu.SMEM((blocks,), jnp.int32)

    def buffers(rows, columns):
        return pltpu.VMEM((BUFFERS, rows, columns), bf16)

    sems = pltpu.SemaphoreType.DMA((BUFFERS,))
    ours, for_core, weighted, pieces, ahead = pl.pallas_call(
        functools.partial(first_kernel, span, width, wide_count, rep_count),
        out_shape=(
            shape((cols, width), f32),
            shape((cols, width), bf16),
            pltpu.VMEM((cols, tokens + step_rows), bf16),
            shape((4, wide_count, lines, width), bf16),
            pltpu.VMEM((2, 4 * step_rows, width), bf16),
        ),
        in_specs=[HBM, HBM, HBM, HBM],
        out_specs=(VMEM,) * 5,
        scratch_shapes=[
            pltpu.SMEM(seq_lengths.shape, jnp.int32),
            table,
            buffers(step_rows, 2 * width),
            buffers(step_rows, cols),
            pltpu.VMEM((cols, step_rows), bf16),
            pltpu.VMEM((cols, step_rows), bf16),
            pltpu.VMEM((cols, 2 * width), f32),
            pltpu.VMEM(hidden.shape, bf16),
            pltpu.VMEM((lines, hidden.shape[2]), f32),
            sems,
            sems,
            pltpu.SemaphoreType.DMA,
            pltpu.SemaphoreType.DMA,
            pltpu.SemaphoreType.DMA((2,)),
        ],
        compiler_params=PARAMS,
        name="first_chunk",
    )(in_hbm(seq_lengths), activations, in_hbm(value_grads), in_hbm(hidden))
    core_part = lax.ppermute(for_core, "rep", core_pairs)
    both_pairs = [(i, i ^ 3) for i in range(rep_count)]
    moved = jnp.stack(
        [
            pieces[0],
            lax.ppermute(pieces[1], "rep", chip_pairs),
            lax.ppermute(pieces[2], "rep", core_pairs),
            lax.ppermute(pieces[3], "rep", both_pairs),
        ]
    )

    for_chip = (ours + core_part.astype(f32)).astype(bf16)
    chip_part = lax.ppermute(for_chip, "rep", chip_pairs)

    def own_call(mine, ahead, order, out_shape):
        return pl.pallas_call(
            functools.partial(own_kernel, span, width, mine),
            out_shape=out_shape,
            in_specs=[SMEM, HBM, VMEM, VMEM, HBM],
            out_specs=(VMEM,) * len(out_shape),
            scratch_shapes=[
                table,
                pltpu.VMEM((3, 4 * step_rows, width), bf16),
                pltpu.VMEM((cols, width), f32),
                pltpu.SemaphoreType.DMA((3,)),
            ]
            + [pltpu.SemaphoreType.DMA((2,))] * (not mine),
            compiler_params=PARAMS,
            name="own_chunk" if mine else "near_chunk",
        )(seq_lengths, activations, weighted, ahead, order)

    for_core, ahead = own_call(
        False, ahead, for_chip, (shape((cols, width), bf16), pltpu.VMEM((2, 4 * step_rows, width), bf16))
    )
    core_part = lax.ppermute(for_core, "rep", core_pairs)
    pieces = [moved[:, 0]]
    for dz in range(1, wide_count):
        pairs = [(i, i ^ dz) for i in range(wide_count)]
        pieces.append(lax.ppermute(moved[:, dz], "wide", pairs))
    moved = jnp.stack(pieces, axis=1)
    group_rows = 2 * wide_count * lines
    hidden_kept = moved[:2].reshape(group_rows, width)
    hidden_sent = moved[2:].reshape(group_rows, width)

    (own_part,) = own_call(True, ahead, for_core, (shape((cols, width), f32),))
    new_master, new_first, new_second, kept, sent = pl.pallas_call(
        update_kernel,
        out_shape=(pltpu.VMEM((width, cols), f32),) * 3
        + (shape((group_rows, cols), f32), shape((group_rows, cols), bf16)),
        in_specs=[VMEM] * 8,
        out_specs=(VMEM,) * 5,
        compiler_params=PARAMS,
        name="update",
    )(own_part, core_part, chip_part, master, first_moment, second_moment, hidden_kept, hidden_sent)
    half = wide_count * lines
    from_chip = lax.ppermute(kept[half:].astype(bf16), "rep", chip_pairs)
    from_both = lax.ppermute(sent[half:], "rep", both_pairs)
    from_core = lax.ppermute(sent[:half], "rep", core_pairs)
    summed = kept[:half] + from_core.astype(f32) + from_chip.astype(f32) + from_both.astype(f32)
    arrived = []
    for place in range(1, wide_count):
        pairs = [(i, i ^ place) for i in range(wide_count)]
        arrived.append(
            lax.ppermute(summed[place * lines : (place + 1) * lines].astype(bf16), "wide", pairs)
        )
    kv_local = cols // HEAD
    rows = (HEADS // KV_HEADS) * lines
    mixed, late, new_master, new_first, new_second = pl.pallas_call(
        attention_kernel,
        out_shape=(
            shape((kv_local, rows, HEAD), f32),
            shape((kv_local, rows, lines), bf16),
            *(pltpu.HBM((width, cols), f32),) * 3,
        ),
        in_specs=[SMEM] + [VMEM] * 7,
        out_specs=(VMEM, VMEM, HBM, HBM, HBM),
        scratch_shapes=[
            pltpu.VMEM((lines, queries.shape[2]), f32),
            pltpu.VMEM((lines, cols), f32),
            pltpu.SemaphoreType.DMA((3,)),
        ],
        compiler_params=PARAMS,
        name="cache_attention",
    )(cache_lengths, queries, new_keys, cache_keys, cache_values, new_master, new_first, new_second)
    new_values, attended = pl.pallas_call(
        functools.partial(finish_kernel, step_count, row_local),
        out_shape=(shape(new_keys.shape, bf16), shape(queries.shape, bf16)),
        in_specs=[VMEM] * (3 + len(arrived)),
        out_specs=(VMEM, VMEM),
        scratch_shapes=[pltpu.VMEM((lines, queries.shape[2]), f32)],
        compiler_params=PARAMS,
        name="finish",
    )(mixed, late, summed[:lines], *arrived)
    return (new_master, new_first, new_second, new_values, attended)


def in_hbm(value):
    return pltpu.with_memory_space_constraint(value, pltpu.HBM)


def dispatch(*args):
    _, value_grads, seq_lengths, master, _, _, hidden = args[:7]
    lines = hidden.shape[0] * hidden.shape[1]
    wide_count = lax.axis_size("wide")
    fits = (
        lax.axis_size("rep") == 4
        and wide_count & (wide_count - 1) == 0
        and master.shape[0] % 128 == 0
        and master.shape[1] % QUANT == 0
        and (value_grads.shape[0] // seq_lengths.shape[0]) % TOKEN_BLOCK == 0
        and lines == 16
        and (value_grads.shape[0] // seq_lengths.shape[0]) & (value_grads.shape[0] // seq_lengths.shape[0] - 1) == 0
        and seq_lengths.shape[0] >= STEP_BLOCKS
        and seq_lengths.shape[0] % STEP_BLOCKS == 0
        and seq_lengths.shape[0] < BUFFERS * STEP_BLOCKS
    )
    if not fits:
        return on_device_plain(*args)
    return on_device(*args)


def solution(mesh):
    in_specs = (
        P("rep", "wide"),
        P("rep", "tp"),
        P("rep"),
        P(("wide", "rep"), "tp"),
        P(("wide", "rep"), "tp"),
        P(("wide", "rep"), "tp"),
        P(None, ("wide", "rep"), None),
        P(None, ("wide", "rep"), "tp"),
        P(None, ("wide", "rep"), "tp"),
        P(("wide", "rep"), None, "tp"),
        P(("wide", "rep"), None, "tp"),
        P(("wide", "rep")),
    )
    out_specs = (
        P(("wide", "rep"), "tp"),
        P(("wide", "rep"), "tp"),
        P(("wide", "rep"), "tp"),
        P(None, ("wide", "rep"), "tp"),
        P(None, ("wide", "rep"), "tp"),
    )
    return jax.shard_map(
        dispatch, mesh=mesh, in_specs=in_specs, out_specs=out_specs, check_vma=False
    )
```
